32 devices in a mesh: band: 4 (over y, x), lev: 8 (over z, core).
Axes of the slice: x: 2, y: 2, z: 4, core: 2. Of those that a mesh axis runs over, the one named last changes fastest.
Arguments:
- adj_spec: bfloat16 [32, 1280, 2, 1280], P('lev', 'band'), may hold values from -6 to 6
- wave_of_slot: int32 [1280], replicated, may hold values from 0 to 1279, each once
- legendre: bfloat16 [1280, 8, 1280], P('band'), may hold values from -0.15625 to 0.15625
- lat_weight: float32 [8], replicated, may hold values from 0.5 to 1.5
- traj: bfloat16 [32, 16, 5136], P('lev', 'band'), may hold values from -3 to 3
- traj_exp: int32 [32, 16, 4], P('lev', 'band'), may hold values from -2 to 2
- traj_order: int32 [8, 4], P('lev'), may hold values from 0 to 3, each once within a row
- lev_coef: float32 [32], P('lev'), may hold values from 0.02 to 0.2
Outputs:
- adj_out: bfloat16 [32, 1280, 2, 1280], P('lev', 'band')
The draws below stay inside these ranges and needn't reach their ends.
Inputs may be any that keep to these rules, and one draw needn't show every extreme that they name: `wave_of_slot`: every wavenumber 0 to 1279 is held by exactly one slot. `traj_order`: each row is a permutation of 0 to 3.
All inputs are finite; a program needn't handle non-finite values.
Results may differ from the reference program's by a relative error of at most 0.0085.
Values may be sent and summed in bfloat16 or wider, within the bound.
A program may use at most 128 MiB of HBM per device.

```python
import math
import jax
import jax.numpy as jnp
from jax import lax

M = 1280
NLON = 5136
NBLK = 4
LEV_DEV = 4
NLAT = 16
NH = 8
NLEV = 32
N_LEV = 8


def touch_ends(values, key, smallest, largest):
    longest = values.shape.index(max(values.shape))
    spots = []
    for shift in (0, 1):
        where = [jax.random.randint(jax.random.fold_in(key, axis), (), 0, length) for axis, length in enumerate(values.shape)]
        where[longest] = (where[longest] + shift) % values.shape[longest]
        spots.append(tuple(where))
    return values.at[spots[0]].set(smallest).at[spots[1]].set(largest)


def levels(stream_key, shape, shards, smallest, top_value):
    loudness = 1.0
    for position, blocks in shards:
        steps = jax.random.uniform(jax.random.fold_in(jax.random.fold_in(stream_key, 6), position), (blocks,), jnp.float32, smallest / len(shards), top_value / len(shards))
        loudness = loudness * jnp.repeat(jnp.exp(steps), shape[position] // blocks).reshape((-1,) + (1,) * (len(shape) - 1 - position))
    return loudness


def noise(own_key, extent, width, bound, cuts=(), held_as=jnp.bfloat16):
    values = jax.random.normal(own_key, extent, jnp.float32) * width
    if len(cuts) > 0:
        values = levels(own_key, extent, cuts, -0.22, 0.18) * values
    return jnp.clip(values, min=-bound, max=bound).astype(held_as)


def setup_inputs(seed: int = 0) -> dict:
    key_list = jax.random.split(jax.random.key(seed), 9)
    adj_spec = noise(key_list[0], (NLEV, M, 2, M), 1.0, 6.0, ((0, 8), (1, 4)))
    wave_of_slot = jax.random.permutation(key_list[1], M).astype(jnp.int32)
    legendre = noise(key_list[2], (M, NH, M), M ** -0.5, 0.15625, ((0, 4),))
    lat_weight = jnp.clip(jax.random.uniform(key_list[3], (NH,), jnp.float32, 0.5, 1.5), 0.5, 1.5)
    traj = noise(key_list[4], (NLEV, NLAT, NLON), 0.5, 3.0, ((0, 8), (1, 4)))
    traj_exp = touch_ends(jax.random.randint(key_list[5], (NLEV, NLAT, NBLK), -2, 3), jax.random.fold_in(key_list[5], 1), -2, 2).astype(jnp.int32)
    traj_order = jax.vmap(lambda own: jax.random.permutation(own, LEV_DEV))(jax.random.split(key_list[6], N_LEV)).reshape((N_LEV, LEV_DEV)).astype(jnp.int32)
    lev_coef = jnp.clip(jnp.exp(math.log(0.2) - 2.3025851 * jax.random.uniform(key_list[7], (NLEV,), jnp.float32) ** levels(key_list[7], (NLEV,), ((0, 8),), -0.2, 0.2)), 0.02, 0.2)
    return {"adj_spec": adj_spec, "wave_of_slot": wave_of_slot, "legendre": legendre, "lat_weight": lat_weight, "traj": traj, "traj_exp": traj_exp, "traj_order": traj_order, "lev_coef": lev_coef}


def trig_block(wave_ids, lon_start, block_width, lon_count):
    lon_ids = lon_start + jnp.arange(block_width, dtype=jnp.int32)
    phase_int = wave_ids.astype(jnp.int32)[:, None] * lon_ids[None, :] % lon_count
    angle_rad = phase_int.astype(jnp.float32) * (2.0 * math.pi / lon_count)
    return jnp.stack([jnp.cos(angle_rad), -jnp.sin(angle_rad)], axis=1).astype(jnp.bfloat16)

def reference(adj_spec, wave_of_slot, legendre, lat_weight, traj, traj_exp, traj_order, lev_coef):
    highest = lax.Precision.HIGHEST
    degree_ids = jnp.arange(M, dtype=jnp.int32)
    valid_mask = degree_ids[None, :] < (M - wave_of_slot.astype(jnp.int32))[:, None]
    masked = jnp.where(valid_mask[None, :, None, :], adj_spec, jnp.zeros_like(adj_spec))
    parity_sign = jnp.where(degree_ids % 2 == 0, 1.0, -1.0).astype(jnp.float32)
    table_full = legendre.astype(jnp.float32)
    weight_q = jnp.repeat(lat_weight, 2)

    def synthesis(level_data):
        values = level_data.astype(jnp.float32)
        stacked = jnp.stack([values, values * parity_sign], axis=2)
        side_values = jnp.einsum('scej,shj->sche', stacked, table_full, precision=highest)
        return (side_values.reshape(M, 2, NLAT) * weight_q).astype(jnp.bfloat16)
    fourier = lax.map(synthesis, masked).astype(jnp.float32)
    block_width = NLON // NBLK
    norm_scale = 1.0 / math.sqrt(M)
    stored = traj.astype(jnp.float32).reshape(N_LEV, LEV_DEV, NLAT, NLON)
    select = (traj_order[:, None, :] == jnp.arange(LEV_DEV, dtype=jnp.int32)[None, :, None]).astype(jnp.float32)
    level_coef = lev_coef[:, None, None]
    analysis = jnp.zeros((NLEV, M, 2, NLAT), jnp.float32)
    for block_id in range(NBLK):
        lon_start = block_id * block_width
        trig_table = trig_block(wave_of_slot, lon_start, block_width, NLON).astype(jnp.float32)
        grid_block = jnp.einsum('lscq,scw->lqw', fourier, trig_table, precision=highest) * norm_scale
        running = jnp.cumsum(grid_block, axis=0)
        above_sum = jnp.concatenate([jnp.zeros_like(grid_block[:1]), running[:-1]], axis=0)
        exponent = jnp.exp2(traj_exp[:, :, block_id].astype(jnp.float32)).reshape(N_LEV, LEV_DEV, NLAT)
        traj_piece = stored[..., lon_start:lon_start + block_width] * exponent[..., None]
        traj_value = jnp.einsum('gir,grqw->giqw', select, traj_piece, precision=highest).reshape(NLEV, NLAT, block_width)
        forcing = ((1.0 + jnp.tanh(traj_value)) * (grid_block + level_coef * above_sum)).astype(jnp.bfloat16).astype(jnp.float32)
        analysis = analysis + jnp.einsum('lqw,scw->lscq', forcing, trig_table, precision=highest) * norm_scale
    halves = analysis.reshape(NLEV, M, 2, NH, 2)
    sym_part = (halves[..., 0] + halves[..., 1]).astype(jnp.bfloat16)
    anti_part = (halves[..., 0] - halves[..., 1]).astype(jnp.bfloat16)

    def analysis_level(level_pair):
        from_sym = jnp.einsum('sch,shj->scj', level_pair[0].astype(jnp.float32), table_full, precision=highest)
        from_anti = jnp.einsum('sch,shj->scj', level_pair[1].astype(jnp.float32), table_full, precision=highest)
        return jnp.where(degree_ids % 2 == 0, from_sym, from_anti)
    result = lax.map(analysis_level, (sym_part, anti_part))
    return jnp.where(valid_mask[None, :, None, :], result, 0.0).astype(jnp.bfloat16)
```

```python
import functools
import math

import jax
import jax.numpy as jnp
from jax import lax
from jax.experimental import pallas as pl
from jax.experimental.pallas import tpu as pltpu
from jax.sharding import PartitionSpec as P

NBLK = 4
LANES = 128
MESH = pl.DeviceIdType.MESH


def slot_step(slots):
    step = 64 if slots % 64 == 0 else slots
    sub = next(width for width in (32, 16, 8, 4, 2, 1) if step % width == 0)
    return step, sub


def split_parity(leg_ref, limit_ref, first, sub):
    table = leg_ref[pl.ds(first, sub)].astype(jnp.float32)
    heights, degrees = table.shape[1], table.shape[2]
    lane = lax.broadcasted_iota(jnp.int32, table.shape, 2)
    limit = jnp.concatenate([limit_ref[pl.ds(first, sub)]] * (degrees // LANES), axis=2)
    table = jnp.where(lane < limit, table, 0.0)
    even = jnp.where(lane % 2 == 0, table, 0.0)
    odd = jnp.where(lane % 2 == 0, 0.0, table)
    rows = sub * heights
    return (
        even.reshape(rows, degrees).astype(jnp.bfloat16),
        odd.reshape(rows, degrees).astype(jnp.bfloat16),
    )


def same_slot(sub, heights, levels):
    shape = (sub, heights, levels * sub * 2)
    held = lax.broadcasted_iota(jnp.int32, shape, 0)
    lane = lax.broadcasted_iota(jnp.int32, shape, 2)
    return held == (lane % (sub * 2)) // 2


def swap_pairs(value):
    lane = lax.broadcasted_iota(jnp.int32, value.shape, 1)
    width = value.shape[1]
    return jnp.where(lane % 2 == 0, pltpu.roll(value, width - 1, 1), pltpu.roll(value, 1, 1))


def synthesis_kernel(step, sub, x_ref, leg_ref, limit_ref, weight_ref, turn_ref, coef_ref, out_ref, total_ref):
    levels, degrees = x_ref.shape[0], x_ref.shape[3]
    heights = leg_ref.shape[1]
    mask = same_slot(sub, heights, levels)
    width = sub * 2
    north, south = [], []
    for first in range(0, step, sub):
        even, odd = split_parity(leg_ref, limit_ref, first, sub)
        spec = x_ref[:, pl.ds(first, sub)].reshape(levels * width, degrees)
        sums = []
        for table in (even, odd):
            cross = lax.dot_general(
                table, spec, (((1,), (1,)), ((), ())), preferred_element_type=jnp.float32
            ).reshape(sub, heights, levels * width)
            sums.append(jnp.sum(jnp.where(mask, cross, 0.0), axis=0))
        north.append(sums[0] + sums[1])
        south.append(sums[0] - sums[1])
    weight = weight_ref[...][:, :1]
    turn = turn_ref[...]
    bands = out_ref.shape[0]
    pairs = heights // bands
    for side, parts in enumerate((north, south)):
        total = None
        for level in range(levels + 1):
            if level < levels:
                lanes = slice(level * width, (level + 1) * width)
                value = jnp.concatenate([part[:, lanes] for part in parts], axis=1) * weight
                value = value * turn[0:1] + swap_pairs(value) * turn[1:2]
                held = value if total is None else value + coef_ref[level] * total
                total = value if total is None else total + value
                first, ref = (side * levels + level) * pairs, out_ref
            else:
                held, first, ref = total, side * pairs, total_ref
            sent = held.astype(jnp.bfloat16)
            for band in range(bands):
                ref[band, first : first + pairs] = sent[band * pairs : (band + 1) * pairs]


def analysis_kernel(step, sub, coef_ref, leg_ref, limit_ref, turn_ref, out_ref):
    levels, degrees = out_ref.shape[0], out_ref.shape[3]
    heights = leg_ref.shape[1]
    mask = same_slot(sub, heights, levels)
    width = sub * 2
    turn = turn_ref[...]
    held = coef_ref[...].astype(jnp.float32)
    bands = held.shape[0]
    pairs = heights // bands
    sides = []
    for side in range(2):
        values = []
        for level in range(levels):
            first = (side * levels + level) * pairs
            value = jnp.concatenate([held[band, first : first + pairs] for band in range(bands)], axis=0)
            values.append(value * turn[0:1] - swap_pairs(value) * turn[1:2])
        sides.append(values)
    for index, first in enumerate(range(0, step, sub)):
        tables = split_parity(leg_ref, limit_ref, first, sub)
        lanes = slice(index * width, (index + 1) * width)
        total = None
        for values, table in zip(sides, tables):
            row = jnp.concatenate([value[:, lanes] for value in values], axis=1)
            spread = jnp.where(mask, row[None], 0.0).reshape(sub * heights, levels * width)
            part = lax.dot_general(
                spread.astype(jnp.bfloat16),
                table,
                (((0,), (0,)), ((), ())),
                preferred_element_type=jnp.float32,
            )
            total = part if total is None else total + part
        out_ref[:, pl.ds(first, sub)] = total.astype(jnp.bfloat16).reshape(levels, sub, 2, degrees)


def spectral_call(kernel, slots, operands, specs, out_shape, out_spec, name):
    step, sub = slot_step(slots)
    return pl.pallas_call(
        functools.partial(kernel, step, sub),
        grid=(slots // step,),
        in_specs=specs,
        out_specs=out_spec,
        out_shape=out_shape,
        name=name,
        compiler_params=pltpu.CompilerParams(vmem_limit_bytes=48 * 1024 * 1024),
    )(*operands)


def cos_turn(count, period):
    left = count - jnp.floor(count * (1.0 / period)) * period
    angle = math.pi * (0.5 - jnp.abs(left * (2.0 / period) - 1.0))
    square = angle * angle
    series = 1.0
    for order in (11, 9, 7, 5, 3):
        series = 1.0 - series * square * (1.0 / (order * (order - 1)))
    return -angle * series


def fill_table(waves_ref, table_ref, lon_count):
    period = 2 * lon_count
    rows = table_ref.shape[0]
    back = 1.5 * lon_count
    row = lax.broadcasted_iota(jnp.int32, (8, LANES), 0).astype(jnp.float32)
    part = lax.broadcasted_iota(jnp.int32, (8, LANES), 1) % 2
    shift = part.astype(jnp.float32) * (lon_count // 2)

    def column(index, carry):
        lanes = pl.ds(pl.multiple_of(index * LANES, LANES), LANES)
        wave = jnp.broadcast_to(waves_ref[0:1, lanes], (8, LANES))
        near = wave * (2.0 * row + 1.0)
        near_cos, near_sin = cos_turn(near, period), cos_turn(near + back, period)
        middle = wave * (16.0 * row)
        middle_cos, middle_sin = cos_turn(middle, period), cos_turn(middle + back, period)
        fine = []
        for j in range(8):
            c, s = middle_cos[j : j + 1], middle_sin[j : j + 1]
            fine.append((near_cos * c - near_sin * s, near_sin * c + near_cos * s))
        for group in range(-(-rows // 512)):
            far = wave * (128.0 * (row + 8.0 * group)) + shift
            far_cos, far_sin = cos_turn(far, period), cos_turn(far + back, period)
            for n in range(8):
                c, s = far_cos[n : n + 1], far_sin[n : n + 1]
                for j in range(0, 8, 2):
                    first = (group * 8 + n) * 64 + j * 8
                    if first < rows:
                        block = [fine[i][0] * c - fine[i][1] * s for i in (j, j + 1)]
                        table_ref[first : first + 16, lanes] = jnp.concatenate(block).astype(jnp.bfloat16)
        return carry

    lax.fori_loop(0, table_ref.shape[1] // LANES, column, 0)


def fill_gain(traj_ref, pick_ref, gain_ref, quarter, scale):
    levels = traj_ref.shape[0]
    lon_count = traj_ref.shape[2]
    rows, padded = gain_ref.shape[1], gain_ref.shape[2]
    stored = jnp.concatenate([traj_ref[r].astype(jnp.float32) for r in range(levels)], axis=0)
    stored = stored.astype(jnp.bfloat16)
    tiles = -(-quarter // LANES)
    turned = lax.broadcasted_iota(jnp.int32, (LANES, LANES), 0)
    turned = turned + lax.broadcasted_iota(jnp.int32, (LANES, LANES), 1) == LANES - 1
    turned = jnp.where(turned, 1.0, 0.0).astype(jnp.bfloat16)
    for block in range(NBLK):
        if block % 2 == 0:
            tile = block * quarter // LANES
            skip = block * quarter - tile * LANES
        else:
            tile = ((block + 1) * quarter - 1) // LANES - (tiles - 1)
            skip = (tile + tiles) * LANES - (block + 1) * quarter
        stop = min((tile + tiles) * LANES, lon_count)
        window = stored[:, tile * LANES : stop]
        if stop < (tile + tiles) * LANES:
            fill = jnp.zeros((rows, (tile + tiles) * LANES - stop), jnp.bfloat16)
            window = jnp.concatenate([window, fill], axis=1)
        value = jnp.dot(pick_ref[block], window, preferred_element_type=jnp.float32)
        if block % 2:
            value = value.astype(jnp.bfloat16)
            stack = [value[:, t * LANES : (t + 1) * LANES] for t in reversed(range(tiles))]
            value = jnp.dot(jnp.concatenate(stack, axis=0), turned, preferred_element_type=jnp.float32)
            value = jnp.concatenate([value[t * rows : (t + 1) * rows] for t in range(tiles)], axis=1)
        value = (1.0 + jnp.tanh(value[:, skip : skip + quarter])) * scale
        gain_ref[block] = jnp.concatenate([value, jnp.zeros((rows, padded - quarter), jnp.float32)], axis=1)


def grid_kernel(
    sizes,
    mine_ref,
    total_ref,
    waves_ref,
    traj_ref,
    pick_ref,
    coef_ref,
    out_ref,
    held_ref,
    sums_ref,
    pair_ref,
    lower_ref,
    back_ref,
    table_ref,
    gain_ref,
    mine_sem,
    held_sem,
    sums_send,
    sums_sem,
    pair_send,
    lower_sem,
    back_send,
    back_sem,
):
    levels, pairs, quarter, scale = sizes
    bands, rows, width = mine_ref.shape
    lon_count = traj_ref.shape[2]
    groups = lower_ref.shape[0]
    band, lev = lax.axis_index("band"), lax.axis_index("lev")
    group, core = lev // 2, lev % 2

    def there(ahead):
        return lax.rem(band + ahead, bands)

    barrier = pltpu.get_barrier_semaphore()
    for ahead in range(bands):
        for side in range(2):
            if ahead or side:
                pl.semaphore_signal(
                    barrier,
                    inc=1,
                    device_id={"band": there(ahead), "lev": group * 2 + (core + side) % 2},
                    device_id_type=MESH,
                )
    for ahead in range(1, groups):
        pl.semaphore_signal(
            barrier,
            inc=1,
            device_id={"band": band, "lev": lax.rem(group + ahead, groups) * 2 + core},
            device_id_type=MESH,
        )
    pl.semaphore_wait(barrier, 2 * bands - 1 + groups - 1)

    sends = []
    for ahead in range(1, bands):
        sends.append(
            pltpu.make_async_remote_copy(
                src_ref=mine_ref.at[there(ahead)],
                dst_ref=held_ref.at[band],
                send_sem=mine_sem.at[ahead],
                recv_sem=held_sem.at[band],
                device_id={"band": there(ahead), "lev": lev},
                device_id_type=MESH,
            )
        )
    for ahead in range(bands):
        for side in range(2):
            if ahead or side:
                sends.append(
                    pltpu.make_async_remote_copy(
                        src_ref=total_ref.at[there(ahead)],
                        dst_ref=sums_ref.at[core, band],
                        send_sem=sums_send.at[side, ahead],
                        recv_sem=sums_sem.at[core, band],
                        device_id={"band": there(ahead), "lev": group * 2 + (core + side) % 2},
                        device_id_type=MESH,
                    )
                )
    for copy in sends:
        copy.start()
    own = [
        pltpu.make_async_copy(mine_ref.at[band], held_ref.at[band], held_sem.at[band]),
        pltpu.make_async_copy(total_ref.at[band], sums_ref.at[core, band], sums_sem.at[core, band]),
    ]
    for copy in own:
        copy.start()

    fill_gain(traj_ref, pick_ref, gain_ref, quarter, scale)

    for source in range(bands):
        for side in range(2):
            pltpu.make_async_copy(
                total_ref.at[source], sums_ref.at[side, source], sums_sem.at[side, source]
            ).wait()
    sums = sums_ref[...].astype(jnp.float32)
    sums = [jnp.concatenate([sums[side, source] for source in range(bands)], axis=1) for side in range(2)]
    pair_ref[...] = (sums[0] + sums[1]).astype(jnp.bfloat16)
    upper = []
    for ahead in range(1, groups):
        copy = pltpu.make_async_remote_copy(
            src_ref=pair_ref,
            dst_ref=lower_ref.at[group],
            send_sem=pair_send.at[ahead],
            recv_sem=lower_sem.at[group],
            device_id={"band": band, "lev": jnp.minimum(group + ahead, groups - 1) * 2 + core},
            device_id_type=MESH,
        )
        upper.append(copy)

        @pl.when(group + ahead < groups)
        def _():
            copy.start()

    fill_table(waves_ref, table_ref, lon_count)

    wave = waves_ref[...]
    part = lax.broadcasted_iota(jnp.int32, wave.shape, 1) % 2
    sign_c = 1.0 - 2.0 * part.astype(jnp.float32)
    sign_m = 1.0 - 2.0 * (wave - 2.0 * jnp.floor(wave * 0.5))
    signs = (sign_m * sign_c, sign_m, sign_c)

    def mirrored(value):
        faces = [value.astype(jnp.float32)] + [value.astype(jnp.float32) * sign for sign in signs]
        return jnp.concatenate(faces, axis=0).astype(jnp.bfloat16)

    def on_grid(value):
        return lax.dot_general(
            mirrored(value), table_ref[...], (((1,), (1,)), ((), ())), preferred_element_type=jnp.float32
        )

    for source in range(bands):
        pltpu.make_async_copy(mine_ref.at[source], held_ref.at[source], held_sem.at[source]).wait()
    grid = on_grid(jnp.concatenate([held_ref[source] for source in range(bands)], axis=1))

    above = jnp.where(core == 1, sums[0], 0.0)
    for below in range(groups - 1):

        @pl.when(below < group)
        def _():
            pltpu.make_async_copy(pair_ref, lower_ref.at[below], lower_sem.at[below]).wait()

        @pl.when(below >= group)
        def _():
            lower_ref[below] = jnp.zeros(lower_ref.shape[1:], jnp.bfloat16)

        above = above + lower_ref[below].astype(jnp.float32)
    scaled = [
        above[side * pairs : (side + 1) * pairs] * coef_ref[level]
        for side in range(2)
        for level in range(levels)
    ]
    grid = grid + on_grid(jnp.concatenate(scaled, axis=0))

    gain = jnp.concatenate([gain_ref[block] for block in range(NBLK)], axis=0)
    forcing = (gain * grid).astype(jnp.bfloat16)
    back = jnp.dot(forcing, table_ref[...], preferred_element_type=jnp.float32)
    total = back[:rows]
    for block, sign in enumerate(signs):
        total = total + back[(block + 1) * rows : (block + 2) * rows] * sign
    total = total * scale
    half = rows // 2
    both = jnp.concatenate([total[:half] + total[half:], total[:half] - total[half:]], axis=0)
    both = both.astype(jnp.bfloat16)
    for target in range(bands):
        back_ref[target] = both[:, target * width : (target + 1) * width]
    returns = [
        pltpu.make_async_remote_copy(
            src_ref=back_ref.at[there(ahead)],
            dst_ref=out_ref.at[band],
            send_sem=back_send.at[ahead],
            recv_sem=back_sem.at[band],
            device_id={"band": there(ahead), "lev": lev},
            device_id_type=MESH,
        )
        for ahead in range(1, bands)
    ]
    for copy in returns:
        copy.start()
    pltpu.make_async_copy(back_ref.at[band], out_ref.at[band], back_sem.at[band]).start()
    for source in range(bands):
        pltpu.make_async_copy(back_ref.at[source], out_ref.at[source], back_sem.at[source]).wait()
    for copy in sends + returns:
        copy.wait_send()
    for ahead, copy in enumerate(upper, 1):

        @pl.when(group + ahead < groups)
        def _():
            copy.wait_send()


def grid_call(mine, total, waves, traj, pick, coef):
    levels, lat_rows, lon_count = traj.shape
    bands, rows, width = mine.shape
    quarter = lon_count // NBLK
    padded = -(-quarter // 16) * 16
    count = waves.shape[1]
    groups = lax.axis_size("lev") // 2
    pairs = lat_rows // 2
    scale = 1.0 / math.sqrt(count // 2)
    vmem = pl.BlockSpec(memory_space=pltpu.VMEM)
    loose = pl.BlockSpec(memory_space=pl.ANY)
    dma = pltpu.SemaphoreType.DMA
    return pl.pallas_call(
        functools.partial(grid_kernel, (levels, pairs, quarter, scale)),
        in_specs=[loose, loose, vmem, vmem, vmem, pl.BlockSpec(memory_space=pltpu.SMEM)],
        out_specs=vmem,
        out_shape=jax.ShapeDtypeStruct(mine.shape, jnp.bfloat16),
        scratch_shapes=[
            pltpu.VMEM(mine.shape, jnp.bfloat16),
            pltpu.VMEM((2,) + total.shape, jnp.bfloat16),
            pltpu.VMEM((total.shape[1], count), jnp.bfloat16),
            pltpu.VMEM((groups, total.shape[1], count), jnp.bfloat16),
            pltpu.VMEM(mine.shape, jnp.bfloat16),
            pltpu.VMEM((padded, count), jnp.bfloat16),
            pltpu.VMEM((NBLK, rows, padded), jnp.float32),
            dma((bands,)),
            dma((bands,)),
            dma((2, bands)),
            dma((2, bands)),
            dma((groups,)),
            dma((groups,)),
            dma((bands,)),
            dma((bands,)),
        ],
        name="grid",
        compiler_params=pltpu.CompilerParams(
            collective_id=0, has_side_effects=True, vmem_limit_bytes=32 * 1024 * 1024
        ),
    )(mine, total, waves, traj, pick, coef)


def body(adj_spec, wave_of_slot, legendre, lat_weight, traj, traj_exp, traj_order, lev_coef):
    levels, slots, _, degrees = adj_spec.shape
    heights = legendre.shape[1]
    lat_rows = traj.shape[1]
    pairs = lat_rows // 2
    lon_count = traj.shape[2]
    quarter = lon_count // NBLK
    step, _ = slot_step(slots)
    bands = heights // pairs

    first_slot = lax.axis_index("band") * slots
    waves_here = lax.dynamic_slice_in_dim(wave_of_slot, first_slot, slots)
    limit = jnp.broadcast_to((degrees - waves_here)[:, None, None], (slots, heights, LANES))
    weight = jnp.broadcast_to(lat_weight[:, None], (heights, LANES))
    half_turn = jnp.repeat(waves_here, 2).astype(jnp.float32) * (math.pi / lon_count)
    part_sign = 1.0 - 2.0 * (jnp.arange(slots * 2, dtype=jnp.int32) % 2).astype(jnp.float32)
    turn = jnp.stack([jnp.cos(half_turn), jnp.sin(half_turn) * part_sign])

    spec_block = pl.BlockSpec((levels, step, 2, degrees), lambda i: (0, i, 0, 0))
    leg_block = pl.BlockSpec((step, heights, degrees), lambda i: (i, 0, 0))
    limit_block = pl.BlockSpec((step, heights, LANES), lambda i: (i, 0, 0))
    turn_block = pl.BlockSpec((2, step * 2), lambda i: (0, i))
    smem = pl.BlockSpec(memory_space=pltpu.SMEM)
    coef_block = pl.BlockSpec((bands, 2 * levels * pairs, step * 2), lambda i: (0, 0, i))
    total_block = pl.BlockSpec((bands, 2 * pairs, step * 2), lambda i: (0, 0, i))
    fourier, totals = spectral_call(
        synthesis_kernel,
        slots,
        (adj_spec, legendre, limit, weight, turn, lev_coef),
        [spec_block, leg_block, limit_block, pl.BlockSpec((heights, LANES), lambda i: (0, 0)), turn_block, smem],
        (
            jax.ShapeDtypeStruct((bands, 2 * levels * pairs, slots * 2), jnp.bfloat16),
            jax.ShapeDtypeStruct((bands, 2 * pairs, slots * 2), jnp.bfloat16),
        ),
        (coef_block, total_block),
        "synthesis",
    )
    waves = jnp.repeat(wave_of_slot, 2).astype(jnp.float32)[None]
    level_ids = jnp.arange(levels, dtype=jnp.int32)
    chosen = traj_order[0][None, :] == level_ids[:, None]
    own_row = jnp.arange(2, dtype=jnp.int32)[:, None] + 2 * jnp.arange(pairs, dtype=jnp.int32)[None, :]
    same_row = own_row[:, :, None] == jnp.arange(lat_rows, dtype=jnp.int32)
    chosen = chosen[None, :, None, :, None] & same_row[:, None, :, None, :]
    scales = jnp.exp2(traj_exp.astype(jnp.float32)).transpose(2, 0, 1)
    pick = jnp.where(chosen[None], scales[:, None, None, None], 0.0).astype(jnp.bfloat16)
    pick = pick.reshape(NBLK, levels * lat_rows, levels * lat_rows)
    returned = grid_call(fourier, totals, waves, traj, pick, lev_coef)
    return spectral_call(
        analysis_kernel,
        slots,
        (returned, legendre, limit, turn),
        [coef_block, leg_block, limit_block, turn_block],
        jax.ShapeDtypeStruct(adj_spec.shape, jnp.bfloat16),
        spec_block,
        "analysis",
    )


def solution(mesh):
    placed = (
        P("lev", "band", None, None),
        P(),
        P("band", None, None),
        P(),
        P("lev", "band", None),
        P("lev", "band", None),
        P("lev", None),
        P("lev"),
    )
    return jax.shard_map(
        body, mesh=mesh, in_specs=placed, out_specs=P("lev", "band", None, None), check_vma=False
    )
```

```python
import functools
import math

import jax
import jax.numpy as jnp
from jax import lax
from jax.experimental import pallas as pl
from jax.experimental.pallas import tpu as pltpu
from jax.sharding import PartitionSpec as P

NBLK = 4
LANES = 128
MESH = pl.DeviceIdType.MESH
MIB = 1024 * 1024
TO_LANES = (((1,), (1,)), ((), ()))
VMEM = pl.BlockSpec(memory_space=pltpu.VMEM)
SMEM = pl.BlockSpec(memory_space=pltpu.SMEM)
LOOSE = pl.BlockSpec(memory_space=pl.ANY)


def in_hbm(value):
    return pltpu.with_memory_space_constraint(value, pltpu.HBM)


def slot_step(slots, heights):
    step = 64 if slots % 64 == 0 else slots
    sub = max(1, 256 // (2 * heights))
    while step % sub:
        sub -= 1
    return step, sub


def iota(shape, dim):
    return lax.broadcasted_iota(jnp.int32, shape, dim)


def swap_pairs(value):
    lane = iota(value.shape, 1)
    width = value.shape[1]
    return jnp.where(lane % 2 == 0, pltpu.roll(value, width - 1, 1), pltpu.roll(value, 1, 1))


def cos_turn(count, period):
    left = count - jnp.floor(count * (1.0 / period)) * period
    angle = math.pi * (0.5 - jnp.abs(left * (2.0 / period) - 1.0))
    square = angle * angle
    series = 1.0
    for order in (11, 9, 7, 5, 3):
        series = 1.0 - series * square * (1.0 / (order * (order - 1)))
    return -angle * series


def own_group(levels, sub, heights):
    shape = (levels * sub * 2, 2 * sub * heights)
    row, lane = iota(shape, 0), iota(shape, 1)
    return (row % (sub * 2)) // 2 == (lane % (sub * heights)) // heights


def chunk_lanes(index, step, slots):
    if step == slots:
        return slice(None)
    return pl.ds(pl.multiple_of(index * (step * 2), step * 2), step * 2)


def half_turn(waves_ref, first, step, lon_count):
    shape = (8, step * 2)
    slot = iota(shape, 1) // 2
    parts = []
    for begin in range(0, step, 8):
        wave = jnp.zeros(shape, jnp.int32)
        for s in range(begin, min(begin + 8, step)):
            wave = jnp.where(slot == s, waves_ref[first + s], wave)
        parts.append(wave)
    wave = sum(parts).astype(jnp.float32)[:1]
    sign = 1.0 - 2.0 * (iota((1, step * 2), 1) % 2).astype(jnp.float32)
    period = 2 * lon_count
    return cos_turn(wave, period), cos_turn(wave + 1.5 * lon_count, period) * sign


def masked_table(leg, limit):
    rows, degrees = leg.shape
    lane = iota((rows, LANES), 1)
    even = (lane % 2 == 0).astype(jnp.int16) == 1
    lane = lane.astype(jnp.int16)
    zero = jnp.zeros((rows, LANES), jnp.bfloat16)
    tiles = []
    for tile in range(0, degrees, LANES):
        part = jnp.where(lane + jnp.int16(tile) < limit, leg[:, tile : tile + LANES], zero)
        tiles.append(jnp.concatenate([jnp.where(even, part, zero), jnp.where(even, zero, part)], axis=0))
    return jnp.concatenate(tiles, axis=1)


def synthesis_kernel(
    lon_count,
    x_hbm,
    leg_hbm,
    waves_hbm,
    weight_hbm,
    coef_hbm,
    out_ref,
    total_ref,
    leg_ref,
    limit_ref,
    turn_ref,
    x_ref,
    kept_ref,
    waves_ref,
    weight_ref,
    coef_ref,
    x_sem,
    leg_sem,
    small_sem,
):
    levels, slots, _, degrees = x_hbm.shape
    heights = leg_hbm.shape[1]
    step, sub = slot_step(slots, heights)
    bands = out_ref.shape[0]
    pairs = heights // bands
    chunks = slots // step
    begin = lax.axis_index("band") * slots

    def copies(index):
        part = pl.ds(index * step, step)
        return (
            pltpu.make_async_copy(x_hbm.at[:, part], x_ref.at[:, part], x_sem.at[index]),
            pltpu.make_async_copy(leg_hbm.at[part], leg_ref.at[part], leg_sem.at[index]),
        )

    small = [
        pltpu.make_async_copy(waves_hbm, waves_ref, small_sem.at[0]),
        pltpu.make_async_copy(weight_hbm, weight_ref, small_sem.at[1]),
        pltpu.make_async_copy(coef_hbm, coef_ref, small_sem.at[2]),
    ]
    for copy in small:
        copy.start()
    for index in range(chunks):
        for copy in copies(index):
            copy.start()

    keep = own_group(levels, sub, heights)
    fold = (2 * heights, 2 * sub * heights)
    side, parity = iota(fold, 0) // heights, iota(fold, 1) // (sub * heights)
    sign = jnp.where(side * parity == 1, -1.0, 1.0)
    fold = jnp.where(iota(fold, 0) % heights == iota(fold, 1) % heights, sign, 0.0).astype(jnp.bfloat16)
    for copy in small:
        copy.wait()
    row = iota((2 * heights, 1), 0) % heights
    weight = jnp.zeros((2 * heights, 1), jnp.float32)
    for h in range(heights):
        weight = jnp.where(row == h, weight_ref[h], weight)

    def prepare(index, carry):
        lanes = chunk_lanes(index, step, slots)
        turn_cos, turn_sin = half_turn(waves_ref, begin + index * step, step, lon_count)
        turn_ref[0:1, lanes] = turn_cos
        turn_ref[1:2, lanes] = turn_sin
        for first in range(0, step, sub):
            here = begin + index * step + first
            limit = [jnp.full((heights, LANES), degrees - waves_ref[here + s], jnp.int32) for s in range(sub)]
            limit_ref[(index * step + first) // sub] = jnp.concatenate(limit, axis=0).astype(jnp.int16)
        return carry

    lax.fori_loop(0, chunks, prepare, 0)

    def multiply(index):
        for number, first in enumerate(range(0, step, sub)):
            local = pl.ds(index * step + first, sub)
            table = masked_table(
                leg_ref[local].reshape(sub * heights, degrees), limit_ref[(index * step + first) // sub]
            )
            spec = x_ref[:, local].reshape(levels * sub * 2, degrees)
            cross = lax.dot_general(spec, table, TO_LANES, preferred_element_type=jnp.float32)
            kept_ref[lax.rem(index, 2), number] = jnp.where(keep, cross, 0.0).astype(jnp.bfloat16)

    def finish(index):
        lanes = chunk_lanes(index, step, slots)
        turn_cos, turn_sin = turn_ref[0:1, lanes], turn_ref[1:2, lanes]
        total = None
        for level in range(levels + 1):
            if level < levels:
                rows = slice(level * sub * 2, (level + 1) * sub * 2)
                value = kept_ref[lax.rem(index, 2), :, rows].reshape(step * 2, 2 * sub * heights)
                value = lax.dot_general(fold, value, TO_LANES, preferred_element_type=jnp.float32) * weight
                value = value * turn_cos + swap_pairs(value) * turn_sin
                held = value if total is None else value + coef_ref[level] * total
                total = value if total is None else total + value
                base, ref = level * pairs, out_ref
            else:
                held, base, ref = total, 0, total_ref
            sent = held.astype(jnp.bfloat16)
            half = ref.shape[1] // 2
            for side in range(2):
                for band in range(bands):
                    first = side * heights + band * pairs
                    start = side * half + base
                    ref[band, start : start + pairs, lanes] = sent[first : first + pairs]

    for copy in copies(0):
        copy.wait()
    multiply(0)

    def chunk(index, carry):
        for copy in copies(index):
            copy.wait()
        multiply(index)
        finish(index - 1)
        return carry

    lax.fori_loop(1, chunks, chunk, 0)
    finish(chunks - 1)


def analysis_kernel(coef_ref, leg_ref, limit_ref, turn_ref, out_hbm, out_ref, part_ref, out_sem):
    levels, slots, _, degrees = out_hbm.shape
    bands = coef_ref.shape[0]
    heights = leg_ref.shape[1]
    pairs = heights // bands
    step, sub = slot_step(slots, heights)
    chunks = slots // step
    keep = own_group(levels, sub, heights)
    tile = (2 * heights, 2 * sub * heights)
    row, lane = iota(tile, 0), iota(tile, 1)
    same = (row % heights == lane % heights) & (row // heights == lane // (sub * heights))
    tile = jnp.where(same, 1.0, 0.0).astype(jnp.bfloat16)

    def copy(index):
        part = pl.ds(index * step, step)
        return pltpu.make_async_copy(out_ref.at[:, part], out_hbm.at[:, part], out_sem.at[index])

    def prepare(index):
        lanes = chunk_lanes(index, step, slots)
        turn_cos, turn_sin = turn_ref[0:1, lanes], turn_ref[1:2, lanes]
        held = coef_ref[:, :, lanes].astype(jnp.float32)
        spread = []
        for level in range(levels):
            value = []
            for side in range(2):
                for band in range(bands):
                    first = (side * levels + level) * pairs
                    value.append(held[band, first : first + pairs])
            value = jnp.concatenate(value, axis=0)
            value = (value * turn_cos - swap_pairs(value) * turn_sin).astype(jnp.bfloat16)
            spread.append(
                lax.dot_general(value, tile, (((0,), (0,)), ((), ())), preferred_element_type=jnp.float32)
            )
        for number, first in enumerate(range(0, step, sub)):
            rows = slice(first * 2, (first + sub) * 2)
            part = jnp.concatenate([value[rows] for value in spread], axis=0)
            part_ref[lax.rem(index, 2), number] = jnp.where(keep, part, 0.0).astype(jnp.bfloat16)

    def multiply(index):
        for number, first in enumerate(range(0, step, sub)):
            local = pl.ds(index * step + first, sub)
            table = masked_table(
                leg_ref[local].reshape(sub * heights, degrees), limit_ref[(index * step + first) // sub]
            )
            total = jnp.dot(part_ref[lax.rem(index, 2), number], table, preferred_element_type=jnp.float32)
            out_ref[:, local] = total.astype(jnp.bfloat16).reshape(levels, sub, 2, degrees)

    prepare(0)

    def chunk(index, carry):
        multiply(index)
        prepare(index + 1)
        copy(index).start()
        return carry

    lax.fori_loop(0, chunks - 1, chunk, 0)
    multiply(chunks - 1)
    copy(chunks - 1).start()
    for index in range(chunks):
        copy(index).wait()


def synthesis_call(adj_spec, legendre, wave_of_slot, lat_weight, lev_coef, bands, lon_count):
    levels, slots, _, degrees = adj_spec.shape
    heights = legendre.shape[1]
    step, sub = slot_step(slots, heights)
    rows = levels * heights * 2 // bands
    chunks = slots // step
    dma = pltpu.SemaphoreType.DMA
    operands = (adj_spec, legendre, wave_of_slot, lat_weight, lev_coef)
    return pl.pallas_call(
        functools.partial(synthesis_kernel, lon_count),
        in_specs=[LOOSE] * 5,
        out_specs=(VMEM,) * 5,
        out_shape=(
            pltpu.VMEM((bands, rows, slots * 2), jnp.bfloat16),
            pltpu.VMEM((bands, rows // levels, slots * 2), jnp.bfloat16),
            pltpu.VMEM(legendre.shape, jnp.bfloat16),
            pltpu.VMEM((slots // sub, sub * heights, LANES), jnp.int16),
            pltpu.VMEM((2, slots * 2), jnp.float32),
        ),
        scratch_shapes=[
            pltpu.VMEM(adj_spec.shape, jnp.bfloat16),
            pltpu.VMEM((2, step // sub, levels * sub * 2, 2 * sub * heights), jnp.bfloat16),
            pltpu.SMEM(wave_of_slot.shape, jnp.int32),
            pltpu.SMEM(lat_weight.shape, jnp.float32),
            pltpu.SMEM(lev_coef.shape, jnp.float32),
            dma((chunks,)),
            dma((chunks,)),
            dma((3,)),
        ],
        name="synthesis",
        compiler_params=pltpu.CompilerParams(vmem_limit_bytes=24 * MIB),
    )(*[in_hbm(value) for value in operands])


def analysis_call(coef, leg, limit, turn, shape):
    levels, slots, _, degrees = shape
    heights = leg.shape[1]
    step, sub = slot_step(slots, heights)
    return pl.pallas_call(
        analysis_kernel,
        in_specs=[VMEM] * 4,
        out_specs=LOOSE,
        out_shape=pltpu.HBM(shape, jnp.bfloat16),
        scratch_shapes=[
            pltpu.VMEM(shape, jnp.bfloat16),
            pltpu.VMEM((2, step // sub, levels * sub * 2, 2 * sub * heights), jnp.bfloat16),
            pltpu.SemaphoreType.DMA((slots // step,)),
        ],
        name="analysis",
        compiler_params=pltpu.CompilerParams(vmem_limit_bytes=20 * MIB),
    )(coef, leg, limit, turn)


def fill_table(waves_ref, table_ref, lon_count):
    period = 2 * lon_count
    rows = table_ref.shape[0]
    back = 1.5 * lon_count
    row = lax.broadcasted_iota(jnp.int32, (8, LANES), 0).astype(jnp.float32)
    part = lax.broadcasted_iota(jnp.int32, (8, LANES), 1) % 2
    shift = part.astype(jnp.float32) * (lon_count // 2)

    def column(index, carry):
        lanes = pl.ds(pl.multiple_of(index * LANES, LANES), LANES)
        wave = jnp.broadcast_to(waves_ref[0:1, lanes], (8, LANES))
        near = wave * (2.0 * row + 1.0)
        near_cos, near_sin = cos_turn(near, period), cos_turn(near + back, period)
        middle = wave * (16.0 * row)
        middle_cos, middle_sin = cos_turn(middle, period), cos_turn(middle + back, period)
        fine = []
        for j in range(8):
            c, s = middle_cos[j : j + 1], middle_sin[j : j + 1]
            fine.append((near_cos * c - near_sin * s, near_sin * c + near_cos * s))
        for group in range(-(-rows // 512)):
            far = wave * (128.0 * (row + 8.0 * group)) + shift
            far_cos, far_sin = cos_turn(far, period), cos_turn(far + back, period)
            for n in range(8):
                c, s = far_cos[n : n + 1], far_sin[n : n + 1]
                for j in range(0, 8, 2):
                    first = (group * 8 + n) * 64 + j * 8
                    if first < rows:
                        block = [fine[i][0] * c - fine[i][1] * s for i in (j, j + 1)]
                        table_ref[first : first + 16, lanes] = jnp.concatenate(block).astype(jnp.bfloat16)
        return carry

    lax.fori_loop(0, table_ref.shape[1] // LANES, column, 0)


def fill_waves(order_ref, waves_ref):
    wave = order_ref[...].astype(jnp.float32).reshape(order_ref.shape[0] // LANES, LANES)
    high = jnp.floor(wave * (1.0 / 256.0))
    digits = (high.astype(jnp.bfloat16), (wave - 256.0 * high).astype(jnp.bfloat16))
    for half in range(2):
        source = iota((LANES, LANES), 1) // 2 + half * (LANES // 2)
        twice = jnp.where(iota((LANES, LANES), 0) == source, 1.0, 0.0).astype(jnp.bfloat16)
        high, low = [jnp.dot(digit, twice, preferred_element_type=jnp.float32) for digit in digits]
        value = high * 256.0 + low
        for r in range(wave.shape[0]):
            first = (2 * r + half) * LANES
            waves_ref[0:1, first : first + LANES] = value[r : r + 1]


def fill_gain(traj_ref, exp_ref, order_ref, gain_ref, scale):
    levels, lat_rows, lon_count = traj_ref.shape
    quarter = lon_count // NBLK
    half = quarter // 2
    rows = levels * lat_rows
    pairs = lat_rows // 2
    padded = gain_ref.shape[1]
    stored = jnp.concatenate([traj_ref[r].astype(jnp.float32) for r in range(levels)], axis=0)
    stored = stored.astype(jnp.bfloat16)
    turned = iota((LANES, LANES), 0) + iota((LANES, LANES), 1) == LANES - 1
    turned = jnp.where(turned, 1.0, 0.0).astype(jnp.bfloat16)
    row, column = iota((rows, rows), 0), iota((rows, rows), 1)
    held = jnp.zeros((rows, rows), jnp.int32)
    for r in range(levels):
        held = jnp.where(column // lat_rows == r, order_ref[0, r], held)
    lat = 2 * (row % pairs) + row // (levels * pairs)
    hit = (held == row // pairs % levels) & (column % lat_rows == lat)
    for block in range(NBLK):
        power = jnp.zeros((rows, rows), jnp.int32)
        for r in range(levels):
            for q in range(lat_rows):
                power = jnp.where(column == r * lat_rows + q, exp_ref[r, q, block], power)
        factor = jnp.where(power < 0, jnp.where(power == -1, 0.5, 0.25), jnp.where(power == 0, 1.0, 2.0))
        factor = jnp.where(power == 2, 4.0, factor)
        pick = jnp.where(hit, factor, 0.0).astype(jnp.bfloat16)
        for reverse in range(2):
            if reverse:
                last = (block + 1) * quarter - 1
                stop = last // LANES + 1
                skip = stop * LANES - 1 - last
                tiles = -(-(skip + half) // LANES)
                tile = stop - tiles
            else:
                tile = block * quarter // LANES
                skip = block * quarter - tile * LANES
                tiles = -(-(skip + half) // LANES)
                stop = tile + tiles
            window = stored[:, tile * LANES : min(stop * LANES, lon_count)]
            if stop * LANES > lon_count:
                fill = jnp.zeros((rows, stop * LANES - lon_count), jnp.bfloat16)
                window = jnp.concatenate([window, fill], axis=1)
            value = jnp.dot(pick, window, preferred_element_type=jnp.float32)
            if reverse:
                value = value.astype(jnp.bfloat16)
                stack = [value[:, t * LANES : (t + 1) * LANES] for t in reversed(range(tiles))]
                value = jnp.dot(jnp.concatenate(stack, axis=0), turned, preferred_element_type=jnp.float32)
                value = jnp.concatenate([value[t * rows : (t + 1) * rows] for t in range(tiles)], axis=1)
            value = (1.0 + jnp.tanh(value[:, skip : skip + half])) * scale
            face = block + (NBLK if (block + reverse) % 2 else 0)
            value = jnp.concatenate([value, jnp.zeros((rows, padded - half), jnp.float32)], axis=1)
            gain_ref[face * rows : (face + 1) * rows] = value


def grid_kernel(
    sizes,
    mine_ref,
    total_ref,
    wave_of_ref,
    traj_ref,
    exp_ref,
    order_ref,
    coef_ref,
    out_ref,
    held_ref,
    sums_ref,
    pair_ref,
    lower_ref,
    back_ref,
    waves_ref,
    table_ref,
    gain_ref,
    mine_sem,
    held_sem,
    sums_send,
    sums_sem,
    pair_send,
    lower_sem,
    back_send,
    back_sem,
):
    levels, pairs, scale = sizes
    bands, rows, width = mine_ref.shape
    lon_count = traj_ref.shape[2]
    groups = lower_ref.shape[0]
    band, lev = lax.axis_index("band"), lax.axis_index("lev")
    group, core = lev // 2, lev % 2

    def there(ahead):
        return lax.rem(band + ahead, bands)

    barrier = pltpu.get_barrier_semaphore()
    for ahead in range(bands):
        for side in range(2):
            if ahead or side:
                pl.semaphore_signal(
                    barrier,
                    inc=1,
                    device_id={"band": there(ahead), "lev": group * 2 + (core + side) % 2},
                    device_id_type=MESH,
                )
    for ahead in range(1, groups):
        pl.semaphore_signal(
            barrier,
            inc=1,
            device_id={"band": band, "lev": lax.rem(group + ahead, groups) * 2 + core},
            device_id_type=MESH,
        )
    pl.semaphore_wait(barrier, 2 * bands - 1 + groups - 1)

    sends = []
    for ahead in range(1, bands):
        sends.append(
            pltpu.make_async_remote_copy(
                src_ref=mine_ref.at[there(ahead)],
                dst_ref=held_ref.at[band],
                send_sem=mine_sem.at[ahead],
                recv_sem=held_sem.at[band],
                device_id={"band": there(ahead), "lev": lev},
                device_id_type=MESH,
            )
        )
    for ahead in range(bands):
        for side in range(2):
            if ahead or side:
                sends.append(
                    pltpu.make_async_remote_copy(
                        src_ref=total_ref.at[there(ahead)],
                        dst_ref=sums_ref.at[core, band],
                        send_sem=sums_send.at[side, ahead],
                        recv_sem=sums_sem.at[core, band],
                        device_id={"band": there(ahead), "lev": group * 2 + (core + side) % 2},
                        device_id_type=MESH,
                    )
                )
    for copy in sends:
        copy.start()
    own = [
        pltpu.make_async_copy(mine_ref.at[band], held_ref.at[band], held_sem.at[band]),
        pltpu.make_async_copy(total_ref.at[band], sums_ref.at[core, band], sums_sem.at[core, band]),
    ]
    for copy in own:
        copy.start()

    fill_gain(traj_ref, exp_ref, order_ref, gain_ref, scale)
    fill_waves(wave_of_ref, waves_ref)

    for source in range(bands):
        for side in range(2):
            pltpu.make_async_copy(
                total_ref.at[source], sums_ref.at[side, source], sums_sem.at[side, source]
            ).wait()
    sums = sums_ref[...].astype(jnp.float32)
    sums = [jnp.concatenate([sums[side, source] for source in range(bands)], axis=1) for side in range(2)]
    pair_ref[...] = (sums[0] + sums[1]).astype(jnp.bfloat16)
    upper = []
    for ahead in range(1, groups):
        copy = pltpu.make_async_remote_copy(
            src_ref=pair_ref,
            dst_ref=lower_ref.at[group],
            send_sem=pair_send.at[ahead],
            recv_sem=lower_sem.at[group],
            device_id={"band": band, "lev": jnp.minimum(group + ahead, groups - 1) * 2 + core},
            device_id_type=MESH,
        )
        upper.append(copy)

        @pl.when(group + ahead < groups)
        def _():
            copy.start()

    fill_table(waves_ref, table_ref, lon_count)

    wave = waves_ref[...]
    part = iota(wave.shape, 1) % 2
    sign_c = 1.0 - 2.0 * part.astype(jnp.float32)
    sign_m = 1.0 - 2.0 * (wave - 2.0 * jnp.floor(wave * 0.5))
    phase = wave - 4.0 * jnp.floor(wave * 0.25)
    stay = jnp.where(phase == 0.0, sign_c, jnp.where(phase == 2.0, -sign_c, 0.0))
    move = jnp.where(phase == 1.0, -1.0, jnp.where(phase == 3.0, 1.0, 0.0))
    signs = (sign_m * sign_c, sign_m, sign_c)

    for source in range(bands):
        pltpu.make_async_copy(mine_ref.at[source], held_ref.at[source], held_sem.at[source]).wait()
    above = jnp.where(core == 1, sums[0], 0.0)
    for below in range(groups - 1):

        @pl.when(below < group)
        def _():
            pltpu.make_async_copy(pair_ref, lower_ref.at[below], lower_sem.at[below]).wait()

        @pl.when(below >= group)
        def _():
            lower_ref[below] = jnp.zeros(lower_ref.shape[1:], jnp.bfloat16)

        above = above + lower_ref[below].astype(jnp.float32)
    scaled = [
        above[side * pairs : (side + 1) * pairs] * coef_ref[level]
        for side in range(2)
        for level in range(levels)
    ]
    value = jnp.concatenate([held_ref[source] for source in range(bands)], axis=1).astype(jnp.float32)
    value = value + jnp.concatenate(scaled, axis=0)
    same, other = value * stay, swap_pairs(value) * move
    far, near = same + other, same - other
    faces = [value] + [value * sign for sign in signs]
    faces += [far, near * signs[0], far * signs[1], near * signs[2]]
    faces = jnp.concatenate([face.astype(jnp.bfloat16) for face in faces], axis=0)
    grid = lax.dot_general(faces, table_ref[...], TO_LANES, preferred_element_type=jnp.float32)
    forcing = (gain_ref[...] * grid).astype(jnp.bfloat16)
    back = jnp.dot(forcing, table_ref[...], preferred_element_type=jnp.float32)
    back = [back[face * rows : (face + 1) * rows] for face in range(2 * NBLK)]
    total = back[0] + back[1] * signs[0] + back[2] * signs[1] + back[3] * signs[2]
    even = back[4] + back[6] * signs[1]
    odd = back[5] * signs[0] + back[7] * signs[2]
    total = total + (even + odd) * stay + swap_pairs(even - odd) * move
    total = total * scale
    half = rows // 2
    both = jnp.concatenate([total[:half] + total[half:], total[:half] - total[half:]], axis=0)
    both = both.astype(jnp.bfloat16)
    for target in range(bands):
        back_ref[target] = both[:, target * width : (target + 1) * width]
    returns = [
        pltpu.make_async_remote_copy(
            src_ref=back_ref.at[there(ahead)],
            dst_ref=out_ref.at[band],
            send_sem=back_send.at[ahead],
            recv_sem=back_sem.at[band],
            device_id={"band": there(ahead), "lev": lev},
            device_id_type=MESH,
        )
        for ahead in range(1, bands)
    ]
    for copy in returns:
        copy.start()
    pltpu.make_async_copy(back_ref.at[band], out_ref.at[band], back_sem.at[band]).start()
    for source in range(bands):
        pltpu.make_async_copy(back_ref.at[source], out_ref.at[source], back_sem.at[source]).wait()
    for copy in sends + returns:
        copy.wait_send()
    for ahead, copy in enumerate(upper, 1):

        @pl.when(group + ahead < groups)
        def _():
            copy.wait_send()


def grid_call(mine, total, waves, traj, traj_exp, traj_order, coef):
    levels, lat_rows, lon_count = traj.shape
    bands, rows, width = mine.shape
    half = lon_count // (2 * NBLK)
    padded = -(-half // 16) * 16
    count = bands * width
    groups = lax.axis_size("lev") // 2
    pairs = lat_rows // 2
    scale = 1.0 / math.sqrt(count // 2)
    dma = pltpu.SemaphoreType.DMA
    return pl.pallas_call(
        functools.partial(grid_kernel, (levels, pairs, scale)),
        in_specs=[LOOSE, LOOSE, VMEM, VMEM, SMEM, SMEM, SMEM],
        out_specs=VMEM,
        out_shape=pltpu.VMEM(mine.shape, jnp.bfloat16),
        scratch_shapes=[
            pltpu.VMEM(mine.shape, jnp.bfloat16),
            pltpu.VMEM((2,) + total.shape, jnp.bfloat16),
            pltpu.VMEM((total.shape[1], count), jnp.bfloat16),
            pltpu.VMEM((groups, total.shape[1], count), jnp.bfloat16),
            pltpu.VMEM(mine.shape, jnp.bfloat16),
            pltpu.VMEM((1, count), jnp.float32),
            pltpu.VMEM((padded, count), jnp.bfloat16),
            pltpu.VMEM((2 * NBLK * rows, padded), jnp.float32),
            dma((bands,)),
            dma((bands,)),
            dma((2, bands)),
            dma((2, bands)),
            dma((groups,)),
            dma((groups,)),
            dma((bands,)),
            dma((bands,)),
        ],
        name="grid",
        compiler_params=pltpu.CompilerParams(
            collective_id=0, has_side_effects=True, vmem_limit_bytes=24 * MIB
        ),
    )(mine, total, waves, traj, traj_exp, traj_order, coef)


def body(adj_spec, wave_of_slot, legendre, lat_weight, traj, traj_exp, traj_order, lev_coef):
    bands = lax.axis_size("band")
    lon_count = traj.shape[2]
    fourier, totals, leg, limit, turn = synthesis_call(
        adj_spec, legendre, wave_of_slot, lat_weight, lev_coef, bands, lon_count
    )
    coef = grid_call(fourier, totals, wave_of_slot, traj, traj_exp, traj_order, lev_coef)
    return analysis_call(coef, leg, limit, turn, adj_spec.shape)


def solution(mesh):
    placed = (
        P("lev", "band", None, None),
        P(),
        P("band", None, None),
        P(),
        P("lev", "band", None),
        P("lev", "band", None),
        P("lev", None),
        P("lev"),
    )
    return jax.shard_map(
        body, mesh=mesh, in_specs=placed, out_specs=P("lev", "band", None, None), check_vma=False
    )
```

```python
import functools
import math

import jax
import jax.numpy as jnp
from jax import lax
from jax.experimental import pallas as pl
from jax.experimental.pallas import tpu as pltpu
from jax.sharding import PartitionSpec as P

NBLK = 4
LANES = 128
MESH = pl.DeviceIdType.MESH
MIB = 1024 * 1024
TO_LANES = (((1,), (1,)), ((), ()))
VMEM = pl.BlockSpec(memory_space=pltpu.VMEM)
SMEM = pl.BlockSpec(memory_space=pltpu.SMEM)
LOOSE = pl.BlockSpec(memory_space=pl.ANY)


def in_hbm(value):
    return pltpu.with_memory_space_constraint(value, pltpu.HBM)


def slot_step(slots, heights):
    step = 64 if slots % 64 == 0 else slots
    sub = max(1, 256 // (2 * heights))
    while step % sub:
        sub -= 1
    return step, sub


def iota(shape, dim):
    return lax.broadcasted_iota(jnp.int32, shape, dim)


def swap_pairs(value):
    lane = iota(value.shape, 1)
    width = value.shape[1]
    return jnp.where(lane % 2 == 0, pltpu.roll(value, width - 1, 1), pltpu.roll(value, 1, 1))


def cos_turn(count, period):
    left = count - jnp.floor(count * (1.0 / period)) * period
    angle = math.pi * (0.5 - jnp.abs(left * (2.0 / period) - 1.0))
    square = angle * angle
    series = 1.0
    for order in (11, 9, 7, 5, 3):
        series = 1.0 - series * square * (1.0 / (order * (order - 1)))
    return -angle * series


def own_group(levels, sub, heights):
    shape = (levels * sub * 2, 2 * sub * heights)
    row, lane = iota(shape, 0), iota(shape, 1)
    return (row % (sub * 2)) // 2 == (lane % (sub * heights)) // heights


def chunk_lanes(index, step, slots):
    if step == slots:
        return slice(None)
    return pl.ds(pl.multiple_of(index * (step * 2), step * 2), step * 2)


def half_turn(waves_ref, first, step, lon_count):
    shape = (8, step * 2)
    slot = iota(shape, 1) // 2
    parts = []
    for begin in range(0, step, 8):
        wave = jnp.zeros(shape, jnp.int32)
        for s in range(begin, min(begin + 8, step)):
            wave = jnp.where(slot == s, waves_ref[first + s], wave)
        parts.append(wave)
    wave = sum(parts).astype(jnp.float32)[:1]
    sign = 1.0 - 2.0 * (iota((1, step * 2), 1) % 2).astype(jnp.float32)
    period = 2 * lon_count
    return cos_turn(wave, period), cos_turn(wave + 1.5 * lon_count, period) * sign


def masked_table(leg, limit):
    rows, degrees = leg.shape
    lane = iota((rows, LANES), 1)
    even = (lane % 2 == 0).astype(jnp.int16) == 1
    lane = lane.astype(jnp.int16)
    zero = jnp.zeros((rows, LANES), jnp.bfloat16)
    tiles = []
    for tile in range(0, degrees, LANES):
        part = jnp.where(lane + jnp.int16(tile) < limit, leg[:, tile : tile + LANES], zero)
        tiles.append(jnp.concatenate([jnp.where(even, part, zero), jnp.where(even, zero, part)], axis=0))
    return jnp.concatenate(tiles, axis=1)


def synthesize(
    lon_count, out_ref, total_ref, leg_ref, limit_ref, turn_ref, x_ref, kept_ref, waves_ref, weight_ref, coef_ref, start, arrive, first, shadow
):
    levels, slots, _, degrees = x_ref.shape
    heights = leg_ref.shape[1]
    step, sub = slot_step(slots, heights)
    bands = out_ref.shape[0]
    pairs = heights // bands
    chunks = slots // step
    begin = lax.axis_index("band") * slots
    depth = min(2, chunks)
    for index in range(depth):
        start(index)
    first()

    keep = own_group(levels, sub, heights)
    fold = (2 * heights, 2 * sub * heights)
    side, parity = iota(fold, 0) // heights, iota(fold, 1) // (sub * heights)
    sign = jnp.where(side * parity == 1, -1.0, 1.0)
    fold = jnp.where(iota(fold, 0) % heights == iota(fold, 1) % heights, sign, 0.0).astype(jnp.bfloat16)
    row = iota((2 * heights, 1), 0) % heights
    weight = jnp.zeros((2 * heights, 1), jnp.float32)
    for h in range(heights):
        weight = jnp.where(row == h, weight_ref[h], weight)

    def prepare(index, carry):
        lanes = chunk_lanes(index, step, slots)
        turn_cos, turn_sin = half_turn(waves_ref, begin + index * step, step, lon_count)
        turn_ref[0:1, lanes] = turn_cos
        turn_ref[1:2, lanes] = turn_sin
        for first in range(0, step, sub):
            here = begin + index * step + first
            limit = [jnp.full((heights, LANES), degrees - waves_ref[here + s], jnp.int32) for s in range(sub)]
            limit_ref[(index * step + first) // sub] = jnp.concatenate(limit, axis=0).astype(jnp.int16)
        return carry

    lax.fori_loop(0, chunks, prepare, 0)
    shadow()

    def multiply(index):
        for number, first in enumerate(range(0, step, sub)):
            local = pl.ds(index * step + first, sub)
            table = masked_table(
                leg_ref[local].reshape(sub * heights, degrees), limit_ref[(index * step + first) // sub]
            )
            spec = x_ref[:, local].reshape(levels * sub * 2, degrees)
            cross = lax.dot_general(spec, table, TO_LANES, preferred_element_type=jnp.float32)
            kept_ref[lax.rem(index, 2), number] = jnp.where(keep, cross, 0.0).astype(jnp.bfloat16)

    def finish(index):
        lanes = chunk_lanes(index, step, slots)
        turn_cos, turn_sin = turn_ref[0:1, lanes], turn_ref[1:2, lanes]
        total = None
        for level in range(levels + 1):
            if level < levels:
                rows = slice(level * sub * 2, (level + 1) * sub * 2)
                value = kept_ref[lax.rem(index, 2), :, rows].reshape(step * 2, 2 * sub * heights)
                value = lax.dot_general(fold, value, TO_LANES, preferred_element_type=jnp.float32) * weight
                value = value * turn_cos + swap_pairs(value) * turn_sin
                held = value if total is None else value + coef_ref[level] * total
                total = value if total is None else total + value
                base, ref = level * pairs, out_ref
            else:
                held, base, ref = total, 0, total_ref
            sent = held.astype(jnp.bfloat16)
            half = ref.shape[1] // 2
            for side in range(2):
                for band in range(bands):
                    first = side * heights + band * pairs
                    start = side * half + base
                    ref[band, start : start + pairs, lanes] = sent[first : first + pairs]

    def take(index):
        arrive(index)

        @pl.when(index + depth < chunks)
        def _():
            start(index + depth)

        multiply(index)

    take(0)

    def chunk(index, carry):
        take(index)
        finish(index - 1)
        return carry

    lax.fori_loop(1, chunks, chunk, 0)
    finish(chunks - 1)


def analysis_kernel(coef_ref, leg_ref, limit_ref, turn_ref, out_hbm, out_ref, part_ref, out_sem):
    levels, slots, _, degrees = out_hbm.shape
    bands = coef_ref.shape[0]
    heights = leg_ref.shape[1]
    pairs = heights // bands
    step, sub = slot_step(slots, heights)
    chunks = slots // step
    keep = own_group(levels, sub, heights)
    tile = (2 * heights, 2 * sub * heights)
    row, lane = iota(tile, 0), iota(tile, 1)
    same = (row % heights == lane % heights) & (row // heights == lane // (sub * heights))
    tile = jnp.where(same, 1.0, 0.0).astype(jnp.bfloat16)

    def copy(index):
        part = pl.ds(index * step, step)
        return pltpu.make_async_copy(out_ref.at[:, part], out_hbm.at[:, part], out_sem.at[index])

    def prepare(index):
        lanes = chunk_lanes(index, step, slots)
        turn_cos, turn_sin = turn_ref[0:1, lanes], turn_ref[1:2, lanes]
        held = coef_ref[:, :, lanes].astype(jnp.float32)
        spread = []
        for level in range(levels):
            value = []
            for side in range(2):
                for band in range(bands):
                    first = (side * levels + level) * pairs
                    value.append(held[band, first : first + pairs])
            value = jnp.concatenate(value, axis=0)
            value = (value * turn_cos - swap_pairs(value) * turn_sin).astype(jnp.bfloat16)
            spread.append(
                lax.dot_general(value, tile, (((0,), (0,)), ((), ())), preferred_element_type=jnp.float32)
            )
        for number, first in enumerate(range(0, step, sub)):
            rows = slice(first * 2, (first + sub) * 2)
            part = jnp.concatenate([value[rows] for value in spread], axis=0)
            part_ref[lax.rem(index, 2), number] = jnp.where(keep, part, 0.0).astype(jnp.bfloat16)

    def multiply(index):
        for number, first in enumerate(range(0, step, sub)):
            local = pl.ds(index * step + first, sub)
            table = masked_table(
                leg_ref[local].reshape(sub * heights, degrees), limit_ref[(index * step + first) // sub]
            )
            total = jnp.dot(part_ref[lax.rem(index, 2), number], table, preferred_element_type=jnp.float32)
            out_ref[:, local] = total.astype(jnp.bfloat16).reshape(levels, sub, 2, degrees)

    prepare(0)

    def chunk(index, carry):
        multiply(index)
        prepare(index + 1)
        copy(index).start()
        return carry

    lax.fori_loop(0, chunks - 1, chunk, 0)
    multiply(chunks - 1)
    copy(chunks - 1).start()
    for index in range(chunks):
        copy(index).wait()


def analysis_call(coef, leg, limit, turn, shape):
    levels, slots, _, degrees = shape
    heights = leg.shape[1]
    step, sub = slot_step(slots, heights)
    return pl.pallas_call(
        analysis_kernel,
        in_specs=[VMEM] * 4,
        out_specs=LOOSE,
        out_shape=pltpu.HBM(shape, jnp.bfloat16),
        scratch_shapes=[
            pltpu.VMEM(shape, jnp.bfloat16),
            pltpu.VMEM((2, step // sub, levels * sub * 2, 2 * sub * heights), jnp.bfloat16),
            pltpu.SemaphoreType.DMA((slots // step,)),
        ],
        name="analysis",
        compiler_params=pltpu.CompilerParams(vmem_limit_bytes=20 * MIB),
    )(coef, leg, limit, turn)


def fill_table(waves_ref, table_ref, lon_count):
    period = 2 * lon_count
    rows = table_ref.shape[0]
    back = 1.5 * lon_count
    row = lax.broadcasted_iota(jnp.int32, (8, LANES), 0).astype(jnp.float32)
    part = lax.broadcasted_iota(jnp.int32, (8, LANES), 1) % 2
    shift = part.astype(jnp.float32) * (lon_count // 2)

    def column(index, carry):
        lanes = pl.ds(pl.multiple_of(index * LANES, LANES), LANES)
        wave = jnp.broadcast_to(waves_ref[0:1, lanes], (8, LANES))
        near = wave * (2.0 * row + 1.0)
        near_cos, near_sin = cos_turn(near, period), cos_turn(near + back, period)
        middle = wave * (16.0 * row)
        middle_cos, middle_sin = cos_turn(middle, period), cos_turn(middle + back, period)
        fine = []
        for j in range(8):
            c, s = middle_cos[j : j + 1], middle_sin[j : j + 1]
            fine.append((near_cos * c - near_sin * s, near_sin * c + near_cos * s))
        for group in range(-(-rows // 512)):
            far = wave * (128.0 * (row + 8.0 * group)) + shift
            far_cos, far_sin = cos_turn(far, period), cos_turn(far + back, period)
            for n in range(8):
                c, s = far_cos[n : n + 1], far_sin[n : n + 1]
                for j in range(0, 8, 2):
                    first = (group * 8 + n) * 64 + j * 8
                    if first < rows:
                        block = [fine[i][0] * c - fine[i][1] * s for i in (j, j + 1)]
                        table_ref[first : first + 16, lanes] = jnp.concatenate(block).astype(jnp.bfloat16)
        return carry

    lax.fori_loop(0, table_ref.shape[1] // LANES, column, 0)


def fill_waves(order_ref, waves_ref):
    wave = order_ref[...].astype(jnp.float32).reshape(order_ref.shape[0] // LANES, LANES)
    high = jnp.floor(wave * (1.0 / 256.0))
    digits = (high.astype(jnp.bfloat16), (wave - 256.0 * high).astype(jnp.bfloat16))
    for half in range(2):
        source = iota((LANES, LANES), 1) // 2 + half * (LANES // 2)
        twice = jnp.where(iota((LANES, LANES), 0) == source, 1.0, 0.0).astype(jnp.bfloat16)
        high, low = [jnp.dot(digit, twice, preferred_element_type=jnp.float32) for digit in digits]
        value = high * 256.0 + low
        for r in range(wave.shape[0]):
            first = (2 * r + half) * LANES
            waves_ref[0:1, first : first + LANES] = value[r : r + 1]


def fill_gain(traj_ref, exp_ref, order_ref, gain_ref, scale):
    levels, lat_rows, lon_count = traj_ref.shape
    quarter = lon_count // NBLK
    half = quarter // 2
    rows = levels * lat_rows
    pairs = lat_rows // 2
    padded = gain_ref.shape[1]
    stored = jnp.concatenate([traj_ref[r].astype(jnp.float32) for r in range(levels)], axis=0)
    stored = stored.astype(jnp.bfloat16)
    turned = iota((LANES, LANES), 0) + iota((LANES, LANES), 1) == LANES - 1
    turned = jnp.where(turned, 1.0, 0.0).astype(jnp.bfloat16)
    row, column = iota((rows, rows), 0), iota((rows, rows), 1)
    held = jnp.zeros((rows, rows), jnp.int32)
    for r in range(levels):
        held = jnp.where(column // lat_rows == r, order_ref[0, r], held)
    lat = 2 * (row % pairs) + row // (levels * pairs)
    hit = (held == row // pairs % levels) & (column % lat_rows == lat)
    for block in range(NBLK):
        power = jnp.zeros((rows, rows), jnp.int32)
        for r in range(levels):
            for q in range(lat_rows):
                power = jnp.where(column == r * lat_rows + q, exp_ref[r, q, block], power)
        factor = jnp.where(power < 0, jnp.where(power == -1, 0.5, 0.25), jnp.where(power == 0, 1.0, 2.0))
        factor = jnp.where(power == 2, 4.0, factor)
        pick = jnp.where(hit, factor, 0.0).astype(jnp.bfloat16)
        for reverse in range(2):
            if reverse:
                last = (block + 1) * quarter - 1
                stop = last // LANES + 1
                skip = stop * LANES - 1 - last
                tiles = -(-(skip + half) // LANES)
                tile = stop - tiles
            else:
                tile = block * quarter // LANES
                skip = block * quarter - tile * LANES
                tiles = -(-(skip + half) // LANES)
                stop = tile + tiles
            window = stored[:, tile * LANES : min(stop * LANES, lon_count)]
            if stop * LANES > lon_count:
                fill = jnp.zeros((rows, stop * LANES - lon_count), jnp.bfloat16)
                window = jnp.concatenate([window, fill], axis=1)
            value = jnp.dot(pick, window, preferred_element_type=jnp.float32)
            if reverse:
                value = value.astype(jnp.bfloat16)
                stack = [value[:, t * LANES : (t + 1) * LANES] for t in reversed(range(tiles))]
                value = jnp.dot(jnp.concatenate(stack, axis=0), turned, preferred_element_type=jnp.float32)
                value = jnp.concatenate([value[t * rows : (t + 1) * rows] for t in range(tiles)], axis=1)
            value = (1.0 + jnp.tanh(value[:, skip : skip + half])) * scale
            face = block + (NBLK if (block + reverse) % 2 else 0)
            value = jnp.concatenate([value, jnp.zeros((rows, padded - half), jnp.float32)], axis=1)
            gain_ref[face * rows : (face + 1) * rows] = value


def grid_kernel(
    sizes,
    x_hbm,
    leg_hbm,
    wave_hbm,
    traj_hbm,
    weight_hbm,
    exp_hbm,
    order_hbm,
    coef_hbm,
    out_ref,
    leg_ref,
    limit_ref,
    turn_ref,
    x_ref,
    kept_ref,
    mine_ref,
    total_ref,
    wave_of_ref,
    traj_ref,
    slot_ref,
    weight_ref,
    exp_ref,
    order_ref,
    coef_ref,
    held_ref,
    sums_ref,
    pair_ref,
    lower_ref,
    back_ref,
    waves_ref,
    table_ref,
    gain_ref,
    x_sem,
    leg_sem,
    small_sem,
    mine_sem,
    held_sem,
    sums_send,
    sums_sem,
    pair_send,
    lower_sem,
    back_send,
    back_sem,
):
    levels, pairs, scale = sizes
    bands, rows, width = mine_ref.shape
    lon_count = traj_ref.shape[2]
    groups = lower_ref.shape[0]
    band, lev = lax.axis_index("band"), lax.axis_index("lev")
    group, core = lev // 2, lev % 2

    def there(ahead):
        return lax.rem(band + ahead, bands)

    barrier = pltpu.get_barrier_semaphore()
    for ahead in range(bands):
        for side in range(2):
            if ahead or side:
                pl.semaphore_signal(
                    barrier,
                    inc=1,
                    device_id={"band": there(ahead), "lev": group * 2 + (core + side) % 2},
                    device_id_type=MESH,
                )
    for ahead in range(1, groups):
        pl.semaphore_signal(
            barrier,
            inc=1,
            device_id={"band": band, "lev": lax.rem(group + ahead, groups) * 2 + core},
            device_id_type=MESH,
        )
    small = ((wave_hbm, slot_ref), (weight_hbm, weight_ref), (coef_hbm, coef_ref), (wave_hbm, wave_of_ref))
    small += ((traj_hbm, traj_ref), (exp_hbm, exp_ref), (order_hbm, order_ref))
    small = [pltpu.make_async_copy(source, ref, small_sem.at[n]) for n, (source, ref) in enumerate(small)]
    for copy in small:
        copy.start()
    step, _ = slot_step(x_ref.shape[1], leg_ref.shape[1])

    def copies(index):
        part = pl.ds(index * step, step)
        return (
            pltpu.make_async_copy(x_hbm.at[:, part], x_ref.at[:, part], x_sem.at[index]),
            pltpu.make_async_copy(leg_hbm.at[part], leg_ref.at[part], leg_sem.at[index]),
        )

    def start(index):
        for copy in copies(index):
            copy.start()

    def arrive(index):
        for copy in copies(index):
            copy.wait()

    def shadow():
        for copy in small[3:]:
            copy.wait()
        fill_gain(traj_ref, exp_ref, order_ref, gain_ref, scale)
        fill_waves(wave_of_ref, waves_ref)

    def first():
        for copy in small[:3]:
            copy.wait()

    synthesize(
        lon_count,
        mine_ref,
        total_ref,
        leg_ref,
        limit_ref,
        turn_ref,
        x_ref,
        kept_ref,
        slot_ref,
        weight_ref,
        coef_ref,
        start,
        arrive,
        first,
        shadow,
    )
    pl.semaphore_wait(barrier, 2 * bands - 1 + groups - 1)

    sends = []
    for ahead in range(1, bands):
        sends.append(
            pltpu.make_async_remote_copy(
                src_ref=mine_ref.at[there(ahead)],
                dst_ref=held_ref.at[band],
                send_sem=mine_sem.at[ahead],
                recv_sem=held_sem.at[band],
                device_id={"band": there(ahead), "lev": lev},
                device_id_type=MESH,
            )
        )
    for ahead in range(bands):
        for side in range(2):
            if ahead or side:
                sends.append(
                    pltpu.make_async_remote_copy(
                        src_ref=total_ref.at[there(ahead)],
                        dst_ref=sums_ref.at[core, band],
                        send_sem=sums_send.at[side, ahead],
                        recv_sem=sums_sem.at[core, band],
                        device_id={"band": there(ahead), "lev": group * 2 + (core + side) % 2},
                        device_id_type=MESH,
                    )
                )
    for copy in sends:
        copy.start()
    own = [
        pltpu.make_async_copy(mine_ref.at[band], held_ref.at[band], held_sem.at[band]),
        pltpu.make_async_copy(total_ref.at[band], sums_ref.at[core, band], sums_sem.at[core, band]),
    ]
    for copy in own:
        copy.start()

    for source in range(bands):
        for side in range(2):
            pltpu.make_async_copy(
                total_ref.at[source], sums_ref.at[side, source], sums_sem.at[side, source]
            ).wait()
    sums = sums_ref[...].astype(jnp.float32)
    sums = [jnp.concatenate([sums[side, source] for source in range(bands)], axis=1) for side in range(2)]
    pair_ref[...] = (sums[0] + sums[1]).astype(jnp.bfloat16)
    upper = []
    for ahead in range(1, groups):
        copy = pltpu.make_async_remote_copy(
            src_ref=pair_ref,
            dst_ref=lower_ref.at[group],
            send_sem=pair_send.at[ahead],
            recv_sem=lower_sem.at[group],
            device_id={"band": band, "lev": jnp.minimum(group + ahead, groups - 1) * 2 + core},
            device_id_type=MESH,
        )
        upper.append(copy)

        @pl.when(group + ahead < groups)
        def _():
            copy.start()

    fill_table(waves_ref, table_ref, lon_count)

    wave = waves_ref[...]
    part = iota(wave.shape, 1) % 2
    sign_c = 1.0 - 2.0 * part.astype(jnp.float32)
    sign_m = 1.0 - 2.0 * (wave - 2.0 * jnp.floor(wave * 0.5))
    phase = wave - 4.0 * jnp.floor(wave * 0.25)
    stay = jnp.where(phase == 0.0, sign_c, jnp.where(phase == 2.0, -sign_c, 0.0))
    move = jnp.where(phase == 1.0, -1.0, jnp.where(phase == 3.0, 1.0, 0.0))
    signs = (sign_m * sign_c, sign_m, sign_c)

    for source in range(bands):
        pltpu.make_async_copy(mine_ref.at[source], held_ref.at[source], held_sem.at[source]).wait()
    above = jnp.where(core == 1, sums[0], 0.0)
    for below in range(groups - 1):

        @pl.when(below < group)
        def _():
            pltpu.make_async_copy(pair_ref, lower_ref.at[below], lower_sem.at[below]).wait()

        @pl.when(below >= group)
        def _():
            lower_ref[below] = jnp.zeros(lower_ref.shape[1:], jnp.bfloat16)

        above = above + lower_ref[below].astype(jnp.float32)
    scaled = [
        above[side * pairs : (side + 1) * pairs] * coef_ref[level]
        for side in range(2)
        for level in range(levels)
    ]
    value = jnp.concatenate([held_ref[source] for source in range(bands)], axis=1).astype(jnp.float32)
    value = value + jnp.concatenate(scaled, axis=0)
    same, other = value * stay, swap_pairs(value) * move
    far, near = same + other, same - other
    faces = [value] + [value * sign for sign in signs]
    faces += [far, near * signs[0], far * signs[1], near * signs[2]]
    faces = jnp.concatenate([face.astype(jnp.bfloat16) for face in faces], axis=0)
    grid = lax.dot_general(faces, table_ref[...], TO_LANES, preferred_element_type=jnp.float32)
    forcing = (gain_ref[...] * grid).astype(jnp.bfloat16)
    back = jnp.dot(forcing, table_ref[...], preferred_element_type=jnp.float32)
    back = [back[face * rows : (face + 1) * rows] for face in range(2 * NBLK)]
    total = back[0] + back[1] * signs[0] + back[2] * signs[1] + back[3] * signs[2]
    even = back[4] + back[6] * signs[1]
    odd = back[5] * signs[0] + back[7] * signs[2]
    total = total + (even + odd) * stay + swap_pairs(even - odd) * move
    total = total * scale
    half = rows // 2
    both = jnp.concatenate([total[:half] + total[half:], total[:half] - total[half:]], axis=0)
    both = both.astype(jnp.bfloat16)
    for target in range(bands):
        back_ref[target] = both[:, target * width : (target + 1) * width]
    returns = [
        pltpu.make_async_remote_copy(
            src_ref=back_ref.at[there(ahead)],
            dst_ref=out_ref.at[band],
            send_sem=back_send.at[ahead],
            recv_sem=back_sem.at[band],
            device_id={"band": there(ahead), "lev": lev},
            device_id_type=MESH,
        )
        for ahead in range(1, bands)
    ]
    for copy in returns:
        copy.start()
    pltpu.make_async_copy(back_ref.at[band], out_ref.at[band], back_sem.at[band]).start()
    for source in range(bands):
        pltpu.make_async_copy(back_ref.at[source], out_ref.at[source], back_sem.at[source]).wait()
    for copy in sends + returns:
        copy.wait_send()
    for ahead, copy in enumerate(upper, 1):

        @pl.when(group + ahead < groups)
        def _():
            copy.wait_send()


def grid_call(adj_spec, legendre, wave_of_slot, traj, lat_weight, traj_exp, traj_order, lev_coef):
    levels, slots, _, degrees = adj_spec.shape
    heights = legendre.shape[1]
    step, sub = slot_step(slots, heights)
    lat_rows, lon_count = traj.shape[1:]
    bands = lax.axis_size("band")
    groups = lax.axis_size("lev") // 2
    pairs = lat_rows // 2
    rows = levels * lat_rows
    mine = (bands, rows, slots * 2)
    total = (bands, lat_rows, slots * 2)
    count = bands * slots * 2
    half = lon_count // (2 * NBLK)
    padded = -(-half // 16) * 16
    chunks = slots // step
    scale = 1.0 / math.sqrt(count // 2)
    dma = pltpu.SemaphoreType.DMA
    bf16 = jnp.bfloat16
    operands = (adj_spec, legendre, wave_of_slot, traj, lat_weight, traj_exp, traj_order, lev_coef)
    return pl.pallas_call(
        functools.partial(grid_kernel, (levels, pairs, scale)),
        in_specs=[LOOSE] * 8,
        out_specs=(VMEM,) * 4,
        out_shape=(
            pltpu.VMEM(mine, bf16),
            pltpu.VMEM(legendre.shape, bf16),
            pltpu.VMEM((slots // sub, sub * heights, LANES), jnp.int16),
            pltpu.VMEM((2, slots * 2), jnp.float32),
        ),
        scratch_shapes=[
            pltpu.VMEM(adj_spec.shape, bf16),
            pltpu.VMEM((2, step // sub, levels * sub * 2, 2 * sub * heights), bf16),
            pltpu.VMEM(mine, bf16),
            pltpu.VMEM(total, bf16),
            pltpu.VMEM(wave_of_slot.shape, jnp.int32),
            pltpu.VMEM(traj.shape, bf16),
            pltpu.SMEM(wave_of_slot.shape, jnp.int32),
            pltpu.SMEM(lat_weight.shape, jnp.float32),
            pltpu.SMEM(traj_exp.shape, jnp.int32),
            pltpu.SMEM(traj_order.shape, jnp.int32),
            pltpu.SMEM(lev_coef.shape, jnp.float32),
            pltpu.VMEM(mine, bf16),
            pltpu.VMEM((2,) + total, bf16),
            pltpu.VMEM((lat_rows, count), bf16),
            pltpu.VMEM((groups, lat_rows, count), bf16),
            pltpu.VMEM(mine, bf16),
            pltpu.VMEM((1, count), jnp.float32),
            pltpu.VMEM((padded, count), bf16),
            pltpu.VMEM((2 * NBLK * rows, padded), jnp.float32),
            dma((chunks,)),
            dma((chunks,)),
            dma((7,)),
            dma((bands,)),
            dma((bands,)),
            dma((2, bands)),
            dma((2, bands)),
            dma((groups,)),
            dma((groups,)),
            dma((bands,)),
            dma((bands,)),
        ],
        name="grid",
        compiler_params=pltpu.CompilerParams(collective_id=0, has_side_effects=True, vmem_limit_bytes=24 * MIB),
    )(*[in_hbm(value) for value in operands])


def body(adj_spec, wave_of_slot, legendre, lat_weight, traj, traj_exp, traj_order, lev_coef):
    coef, leg, limit, turn = grid_call(
        adj_spec, legendre, wave_of_slot, traj, lat_weight, traj_exp, traj_order, lev_coef
    )
    return analysis_call(coef, leg, limit, turn, adj_spec.shape)


def solution(mesh):
    placed = (
        P("lev", "band", None, None),
        P(),
        P("band", None, None),
        P(),
        P("lev", "band", None),
        P("lev", "band", None),
        P("lev", None),
        P("lev"),
    )
    return jax.shard_map(
        body, mesh=mesh, in_specs=placed, out_specs=P("lev", "band", None, None), check_vma=False
    )
```

```python
import functools
import math

import jax
import jax.numpy as jnp
from jax import lax
from jax.experimental import pallas as pl
from jax.experimental.pallas import tpu as pltpu
from jax.sharding import PartitionSpec as P

NBLK = 4
LANES = 128
MESH = pl.DeviceIdType.MESH
MIB = 1024 * 1024
TO_LANES = (((1,), (1,)), ((), ()))
VMEM = pl.BlockSpec(memory_space=pltpu.VMEM)
SMEM = pl.BlockSpec(memory_space=pltpu.SMEM)
LOOSE = pl.BlockSpec(memory_space=pl.ANY)


def in_hbm(value):
    return pltpu.with_memory_space_constraint(value, pltpu.HBM)


def slot_step(slots, heights):
    step = 64 if slots % 64 == 0 else slots
    sub = max(1, 256 // (2 * heights))
    while step % sub:
        sub -= 1
    return step, sub


def iota(shape, dim):
    return lax.broadcasted_iota(jnp.int32, shape, dim)


def swap_pairs(value):
    lane = iota(value.shape, 1)
    width = value.shape[1]
    return jnp.where(lane % 2 == 0, pltpu.roll(value, width - 1, 1), pltpu.roll(value, 1, 1))


def cos_turn(count, period):
    left = count - jnp.floor(count * (1.0 / period)) * period
    angle = math.pi * (0.5 - jnp.abs(left * (2.0 / period) - 1.0))
    square = angle * angle
    series = 1.0
    for order in (11, 9, 7, 5, 3):
        series = 1.0 - series * square * (1.0 / (order * (order - 1)))
    return -angle * series


def own_group(levels, sub, heights):
    shape = (levels * sub * 2, 2 * sub * heights)
    row, lane = iota(shape, 0), iota(shape, 1)
    return (row % (sub * 2)) // 2 == (lane % (sub * heights)) // heights


def chunk_lanes(index, step, slots):
    if step == slots:
        return slice(None)
    return pl.ds(pl.multiple_of(index * (step * 2), step * 2), step * 2)


def half_turn(waves_ref, first, step, lon_count):
    shape = (8, step * 2)
    slot = iota(shape, 1) // 2
    parts = []
    for begin in range(0, step, 8):
        wave = jnp.zeros(shape, jnp.int32)
        for s in range(begin, min(begin + 8, step)):
            wave = jnp.where(slot == s, waves_ref[first + s], wave)
        parts.append(wave)
    wave = sum(parts).astype(jnp.float32)[:1]
    sign = 1.0 - 2.0 * (iota((1, step * 2), 1) % 2).astype(jnp.float32)
    period = 2 * lon_count
    return cos_turn(wave, period), cos_turn(wave + 1.5 * lon_count, period) * sign


def masked_table(leg, limit):
    rows, degrees = leg.shape
    lane = iota((rows, LANES), 1)
    even = (lane % 2 == 0).astype(jnp.int16) == 1
    lane = lane.astype(jnp.int16)
    zero = jnp.zeros((rows, LANES), jnp.bfloat16)
    tiles = []
    for tile in range(0, degrees, LANES):
        part = jnp.where(lane + jnp.int16(tile) < limit, leg[:, tile : tile + LANES], zero)
        tiles.append(jnp.concatenate([jnp.where(even, part, zero), jnp.where(even, zero, part)], axis=0))
    return jnp.concatenate(tiles, axis=1)


def synthesize(
    lon_count, out_ref, total_ref, leg_ref, limit_ref, turn_ref, x_ref, kept_ref, waves_ref, weight_ref, coef_ref, start, arrive, first, early
):
    levels, slots, _, degrees = x_ref.shape
    heights = leg_ref.shape[1]
    step, sub = slot_step(slots, heights)
    bands = out_ref.shape[0]
    pairs = heights // bands
    chunks = slots // step
    begin = lax.axis_index("band") * slots
    depth = min(2, chunks)
    for index in range(depth):
        start(index)
    first()

    keep = own_group(levels, sub, heights)
    fold = (2 * heights, 2 * sub * heights)
    side, parity = iota(fold, 0) // heights, iota(fold, 1) // (sub * heights)
    sign = jnp.where(side * parity == 1, -1.0, 1.0)
    fold = jnp.where(iota(fold, 0) % heights == iota(fold, 1) % heights, sign, 0.0).astype(jnp.bfloat16)
    row = iota((2 * heights, 1), 0) % heights
    weight = jnp.zeros((2 * heights, 1), jnp.float32)
    for h in range(heights):
        weight = jnp.where(row == h, weight_ref[h], weight)

    def prepare(index):
        lanes = chunk_lanes(index, step, slots)
        turn_cos, turn_sin = half_turn(waves_ref, begin + index * step, step, lon_count)
        turn_ref[0:1, lanes] = turn_cos
        turn_ref[1:2, lanes] = turn_sin
        for first in range(0, step, sub):
            here = begin + index * step + first
            limit = [jnp.full((heights, LANES), degrees - waves_ref[here + s], jnp.int32) for s in range(sub)]
            limit_ref[(index * step + first) // sub] = jnp.concatenate(limit, axis=0).astype(jnp.int16)

    prepare(0)

    def multiply(index):
        for number, first in enumerate(range(0, step, sub)):
            local = pl.ds(index * step + first, sub)
            table = masked_table(
                leg_ref[local].reshape(sub * heights, degrees), limit_ref[(index * step + first) // sub]
            )
            spec = x_ref[:, local].reshape(levels * sub * 2, degrees)
            cross = lax.dot_general(spec, table, TO_LANES, preferred_element_type=jnp.float32)
            kept_ref[lax.rem(index, 2), number] = jnp.where(keep, cross, 0.0).astype(jnp.bfloat16)

    def finish(index):
        lanes = chunk_lanes(index, step, slots)
        turn_cos, turn_sin = turn_ref[0:1, lanes], turn_ref[1:2, lanes]
        total = None
        for level in range(levels + 1):
            if level < levels:
                rows = slice(level * sub * 2, (level + 1) * sub * 2)
                value = kept_ref[lax.rem(index, 2), :, rows].reshape(step * 2, 2 * sub * heights)
                value = lax.dot_general(fold, value, TO_LANES, preferred_element_type=jnp.float32) * weight
                value = value * turn_cos + swap_pairs(value) * turn_sin
                held = value if total is None else value + coef_ref[level] * total
                total = value if total is None else total + value
                base, ref = level * pairs, out_ref
            else:
                held, base, ref = total, 0, total_ref
            sent = held.astype(jnp.bfloat16)
            half = ref.shape[1] // 2
            for side in range(2):
                for band in range(bands):
                    first = side * heights + band * pairs
                    start = side * half + base
                    ref[band, start : start + pairs, lanes] = sent[first : first + pairs]

    def take(index):
        arrive(index)

        @pl.when(index + depth < chunks)
        def _():
            start(index + depth)

        multiply(index)

    take(0)
    if chunks > 1:
        prepare(1)

    def chunk(index, carry):
        take(index)
        prepare(jnp.minimum(index + 1, chunks - 1))
        finish(index - 1)
        return carry

    if chunks > 2:
        lax.fori_loop(1, chunks - 1, chunk, 0)
        early()
        chunk(chunks - 1, 0)
    else:
        lax.fori_loop(1, chunks, chunk, 0)
    finish(chunks - 1)


def total_parts(slots, heights):
    step, _ = slot_step(slots, heights)
    chunks = slots // step
    ends = [0, (chunks - 2) * step * 2, slots * 2] if chunks > 2 else [0, slots * 2]
    return [slice(*pair) for pair in zip(ends, ends[1:])]


def analysis_kernel(coef_ref, leg_ref, limit_ref, turn_ref, out_hbm, out_ref, part_ref, out_sem):
    levels, slots, _, degrees = out_hbm.shape
    bands = coef_ref.shape[0]
    heights = leg_ref.shape[1]
    pairs = heights // bands
    step, sub = slot_step(slots, heights)
    chunks = slots // step
    keep = own_group(levels, sub, heights)
    tile = (2 * heights, 2 * sub * heights)
    row, lane = iota(tile, 0), iota(tile, 1)
    same = (row % heights == lane % heights) & (row // heights == lane // (sub * heights))
    tile = jnp.where(same, 1.0, 0.0).astype(jnp.bfloat16)

    def copy(index):
        part = pl.ds(index * step, step)
        return pltpu.make_async_copy(out_ref.at[:, part], out_hbm.at[:, part], out_sem.at[index])

    def prepare(index):
        lanes = chunk_lanes(index, step, slots)
        turn_cos, turn_sin = turn_ref[0:1, lanes], turn_ref[1:2, lanes]
        held = coef_ref[:, :, lanes].astype(jnp.float32)
        spread = []
        for level in range(levels):
            value = []
            for side in range(2):
                for band in range(bands):
                    first = (side * levels + level) * pairs
                    value.append(held[band, first : first + pairs])
            value = jnp.concatenate(value, axis=0)
            value = (value * turn_cos - swap_pairs(value) * turn_sin).astype(jnp.bfloat16)
            spread.append(
                lax.dot_general(value, tile, (((0,), (0,)), ((), ())), preferred_element_type=jnp.float32)
            )
        for number, first in enumerate(range(0, step, sub)):
            rows = slice(first * 2, (first + sub) * 2)
            part = jnp.concatenate([value[rows] for value in spread], axis=0)
            part_ref[lax.rem(index, 2), number] = jnp.where(keep, part, 0.0).astype(jnp.bfloat16)

    def multiply(index):
        for number, first in enumerate(range(0, step, sub)):
            local = pl.ds(index * step + first, sub)
            table = masked_table(
                leg_ref[local].reshape(sub * heights, degrees), limit_ref[(index * step + first) // sub]
            )
            total = jnp.dot(part_ref[lax.rem(index, 2), number], table, preferred_element_type=jnp.float32)
            out_ref[:, local] = total.astype(jnp.bfloat16).reshape(levels, sub, 2, degrees)

    prepare(0)

    def chunk(index, carry):
        multiply(index)
        prepare(index + 1)
        copy(index).start()
        return carry

    lax.fori_loop(0, chunks - 1, chunk, 0)
    multiply(chunks - 1)
    copy(chunks - 1).start()
    for index in range(chunks):
        copy(index).wait()


def analysis_call(coef, leg, limit, turn, shape):
    levels, slots, _, degrees = shape
    heights = leg.shape[1]
    step, sub = slot_step(slots, heights)
    return pl.pallas_call(
        analysis_kernel,
        in_specs=[VMEM] * 4,
        out_specs=LOOSE,
        out_shape=pltpu.HBM(shape, jnp.bfloat16),
        scratch_shapes=[
            pltpu.VMEM(shape, jnp.bfloat16),
            pltpu.VMEM((2, step // sub, levels * sub * 2, 2 * sub * heights), jnp.bfloat16),
            pltpu.SemaphoreType.DMA((slots // step,)),
        ],
        name="analysis",
        compiler_params=pltpu.CompilerParams(vmem_limit_bytes=20 * MIB),
    )(coef, leg, limit, turn)


def fill_table(waves_ref, table_ref, lon_count):
    period = 2 * lon_count
    rows = table_ref.shape[0]
    back = 1.5 * lon_count
    row = lax.broadcasted_iota(jnp.int32, (8, LANES), 0).astype(jnp.float32)
    part = lax.broadcasted_iota(jnp.int32, (8, LANES), 1) % 2
    shift = part.astype(jnp.float32) * (lon_count // 2)

    def column(index, carry):
        lanes = pl.ds(pl.multiple_of(index * LANES, LANES), LANES)
        wave = jnp.broadcast_to(waves_ref[0:1, lanes], (8, LANES))
        near = wave * (2.0 * row + 1.0)
        near_cos, near_sin = cos_turn(near, period), cos_turn(near + back, period)
        middle = wave * (16.0 * row)
        middle_cos, middle_sin = cos_turn(middle, period), cos_turn(middle + back, period)
        fine = []
        for j in range(8):
            c, s = middle_cos[j : j + 1], middle_sin[j : j + 1]
            fine.append((near_cos * c - near_sin * s, near_sin * c + near_cos * s))
        for group in range(-(-rows // 512)):
            far = wave * (128.0 * (row + 8.0 * group)) + shift
            far_cos, far_sin = cos_turn(far, period), cos_turn(far + back, period)
            for n in range(8):
                c, s = far_cos[n : n + 1], far_sin[n : n + 1]
                for j in range(0, 8, 2):
                    first = (group * 8 + n) * 64 + j * 8
                    if first < rows:
                        block = [fine[i][0] * c - fine[i][1] * s for i in (j, j + 1)]
                        table_ref[first : first + 16, lanes] = jnp.concatenate(block).astype(jnp.bfloat16)
        return carry

    lax.fori_loop(0, table_ref.shape[1] // LANES, column, 0)


def fill_waves(order_ref, waves_ref):
    wave = order_ref[...].astype(jnp.float32).reshape(order_ref.shape[0] // LANES, LANES)
    high = jnp.floor(wave * (1.0 / 256.0))
    digits = (high.astype(jnp.bfloat16), (wave - 256.0 * high).astype(jnp.bfloat16))
    for half in range(2):
        source = iota((LANES, LANES), 1) // 2 + half * (LANES // 2)
        twice = jnp.where(iota((LANES, LANES), 0) == source, 1.0, 0.0).astype(jnp.bfloat16)
        high, low = [jnp.dot(digit, twice, preferred_element_type=jnp.float32) for digit in digits]
        value = high * 256.0 + low
        for r in range(wave.shape[0]):
            first = (2 * r + half) * LANES
            waves_ref[0:1, first : first + LANES] = value[r : r + 1]


def fill_gain(traj_ref, exp_ref, order_ref, gain_ref, scale):
    levels, lat_rows, lon_count = traj_ref.shape
    quarter = lon_count // NBLK
    half = quarter // 2
    rows = levels * lat_rows
    pairs = lat_rows // 2
    padded = gain_ref.shape[1]
    stored = jnp.concatenate([traj_ref[r].astype(jnp.float32) for r in range(levels)], axis=0)
    stored = stored.astype(jnp.bfloat16)
    turned = iota((LANES, LANES), 0) + iota((LANES, LANES), 1) == LANES - 1
    turned = jnp.where(turned, 1.0, 0.0).astype(jnp.bfloat16)
    row, column = iota((rows, rows), 0), iota((rows, rows), 1)
    held = jnp.zeros((rows, rows), jnp.int32)
    for r in range(levels):
        held = jnp.where(column // lat_rows == r, order_ref[0, r], held)
    lat = 2 * (row % pairs) + row // (levels * pairs)
    hit = (held == row // pairs % levels) & (column % lat_rows == lat)
    for block in range(NBLK):
        power = jnp.zeros((rows, rows), jnp.int32)
        for r in range(levels):
            for q in range(lat_rows):
                power = jnp.where(column == r * lat_rows + q, exp_ref[r, q, block], power)
        factor = jnp.where(power < 0, jnp.where(power == -1, 0.5, 0.25), jnp.where(power == 0, 1.0, 2.0))
        factor = jnp.where(power == 2, 4.0, factor)
        pick = jnp.where(hit, factor, 0.0).astype(jnp.bfloat16)
        for reverse in range(2):
            if reverse:
                last = (block + 1) * quarter - 1
                stop = last // LANES + 1
                skip = stop * LANES - 1 - last
                tiles = -(-(skip + half) // LANES)
                tile = stop - tiles
            else:
                tile = block * quarter // LANES
                skip = block * quarter - tile * LANES
                tiles = -(-(skip + half) // LANES)
                stop = tile + tiles
            window = stored[:, tile * LANES : min(stop * LANES, lon_count)]
            if stop * LANES > lon_count:
                fill = jnp.zeros((rows, stop * LANES - lon_count), jnp.bfloat16)
                window = jnp.concatenate([window, fill], axis=1)
            value = jnp.dot(pick, window, preferred_element_type=jnp.float32)
            if reverse:
                value = value.astype(jnp.bfloat16)
                stack = [value[:, t * LANES : (t + 1) * LANES] for t in reversed(range(tiles))]
                value = jnp.dot(jnp.concatenate(stack, axis=0), turned, preferred_element_type=jnp.float32)
                value = jnp.concatenate([value[t * rows : (t + 1) * rows] for t in range(tiles)], axis=1)
            value = (1.0 + jnp.tanh(value[:, skip : skip + half])) * scale
            face = block + (NBLK if (block + reverse) % 2 else 0)
            value = jnp.concatenate([value, jnp.zeros((rows, padded - half), jnp.float32)], axis=1)
            gain_ref[face * rows : (face + 1) * rows] = value


def grid_kernel(
    sizes,
    x_hbm,
    leg_hbm,
    wave_hbm,
    traj_hbm,
    weight_hbm,
    exp_hbm,
    order_hbm,
    coef_hbm,
    out_ref,
    leg_ref,
    limit_ref,
    turn_ref,
    x_ref,
    kept_ref,
    mine_ref,
    total_ref,
    wave_of_ref,
    traj_ref,
    slot_ref,
    weight_ref,
    exp_ref,
    order_ref,
    coef_ref,
    held_ref,
    sums_ref,
    pair_refs,
    lower_refs,
    back_ref,
    waves_ref,
    table_ref,
    gain_ref,
    x_sem,
    leg_sem,
    small_sem,
    mine_sem,
    held_sem,
    sums_send,
    sums_sem,
    pair_send,
    lower_sem,
    back_send,
    back_sem,
):
    levels, pairs, scale = sizes
    bands, rows, width = mine_ref.shape
    lon_count = traj_ref.shape[2]
    groups = lower_refs[0].shape[0]
    parts = total_parts(x_ref.shape[1], leg_ref.shape[1])
    band, lev = lax.axis_index("band"), lax.axis_index("lev")
    group, core = lev // 2, lev % 2

    def there(ahead):
        return lax.rem(band + ahead, bands)

    barrier = pltpu.get_barrier_semaphore()
    for ahead in range(bands):
        for side in range(2):
            if ahead or side:
                pl.semaphore_signal(
                    barrier,
                    inc=1,
                    device_id={"band": there(ahead), "lev": group * 2 + (core + side) % 2},
                    device_id_type=MESH,
                )
    for ahead in range(1, groups):
        pl.semaphore_signal(
            barrier,
            inc=1,
            device_id={"band": band, "lev": lax.rem(group + ahead, groups) * 2 + core},
            device_id_type=MESH,
        )
    small = ((wave_hbm, slot_ref), (weight_hbm, weight_ref), (coef_hbm, coef_ref), (wave_hbm, wave_of_ref))
    small += ((traj_hbm, traj_ref), (exp_hbm, exp_ref), (order_hbm, order_ref))
    small = [pltpu.make_async_copy(source, ref, small_sem.at[n]) for n, (source, ref) in enumerate(small)]
    for copy in small:
        copy.start()
    step, _ = slot_step(x_ref.shape[1], leg_ref.shape[1])

    def copies(index):
        part = pl.ds(index * step, step)
        return (
            pltpu.make_async_copy(x_hbm.at[:, part], x_ref.at[:, part], x_sem.at[index]),
            pltpu.make_async_copy(leg_hbm.at[part], leg_ref.at[part], leg_sem.at[index]),
        )

    def start(index):
        for copy in copies(index):
            copy.start()

    def arrive(index):
        for copy in copies(index):
            copy.wait()

    def shadow():
        for copy in small[3:]:
            copy.wait()
        fill_gain(traj_ref, exp_ref, order_ref, gain_ref, scale)
        fill_waves(wave_of_ref, waves_ref)

    def first():
        for copy in small[:3]:
            copy.wait()

    def totals_out(part):
        lanes = parts[part]
        return [
            pltpu.make_async_remote_copy(
                src_ref=total_ref.at[there(ahead), :, lanes],
                dst_ref=sums_ref.at[core, band, :, lanes],
                send_sem=sums_send.at[part, side, ahead],
                recv_sem=sums_sem.at[part, core, band],
                device_id={"band": there(ahead), "lev": group * 2 + (core + side) % 2},
                device_id_type=MESH,
            )
            for ahead in range(bands)
            for side in range(2)
            if ahead or side
        ]

    def send_totals(part):
        lanes = parts[part]
        for copy in totals_out(part):
            copy.start()
        pltpu.make_async_copy(
            total_ref.at[band, :, lanes], sums_ref.at[core, band, :, lanes], sums_sem.at[part, core, band]
        ).start()

    def upper_out(part):
        return [
            pltpu.make_async_remote_copy(
                src_ref=pair_refs[part],
                dst_ref=lower_refs[part].at[group],
                send_sem=pair_send.at[part, ahead],
                recv_sem=lower_sem.at[part, group],
                device_id={"band": band, "lev": jnp.minimum(group + ahead, groups - 1) * 2 + core},
                device_id_type=MESH,
            )
            for ahead in range(1, groups)
        ]

    def pass_up(part):
        lanes = parts[part]
        for source in range(bands):
            for side in range(2):
                pltpu.make_async_copy(
                    total_ref.at[source, :, lanes], sums_ref.at[side, source, :, lanes], sums_sem.at[part, side, source]
                ).wait()
        pair = []
        for source in range(bands):
            both = [sums_ref[side, source, :, lanes].astype(jnp.float32) for side in range(2)]
            pair.append((both[0] + both[1]).astype(jnp.bfloat16))
        pair_refs[part][...] = jnp.concatenate(pair, axis=1)
        for ahead, copy in enumerate(upper_out(part), 1):

            @pl.when(group + ahead < groups)
            def _():
                copy.start()

    def early():
        pl.semaphore_wait(barrier, 2 * bands - 1 + groups - 1)
        send_totals(0)

    synthesize(
        lon_count,
        mine_ref,
        total_ref,
        leg_ref,
        limit_ref,
        turn_ref,
        x_ref,
        kept_ref,
        slot_ref,
        weight_ref,
        coef_ref,
        start,
        arrive,
        first,
        early,
    )
    if len(parts) == 1:
        early()
    else:
        send_totals(1)
    sends = [
        pltpu.make_async_remote_copy(
            src_ref=mine_ref.at[there(ahead)],
            dst_ref=held_ref.at[band],
            send_sem=mine_sem.at[ahead],
            recv_sem=held_sem.at[band],
            device_id={"band": there(ahead), "lev": lev},
            device_id_type=MESH,
        )
        for ahead in range(1, bands)
    ]
    for copy in sends:
        copy.start()
    pltpu.make_async_copy(mine_ref.at[band], held_ref.at[band], held_sem.at[band]).start()
    if len(parts) > 1:
        pass_up(0)
    shadow()
    pass_up(len(parts) - 1)

    fill_table(waves_ref, table_ref, lon_count)

    wave = waves_ref[...]
    part = iota(wave.shape, 1) % 2
    sign_c = 1.0 - 2.0 * part.astype(jnp.float32)
    sign_m = 1.0 - 2.0 * (wave - 2.0 * jnp.floor(wave * 0.5))
    phase = wave - 4.0 * jnp.floor(wave * 0.25)
    stay = jnp.where(phase == 0.0, sign_c, jnp.where(phase == 2.0, -sign_c, 0.0))
    move = jnp.where(phase == 1.0, -1.0, jnp.where(phase == 3.0, 1.0, 0.0))
    signs = (sign_m * sign_c, sign_m, sign_c)

    for source in range(bands):
        pltpu.make_async_copy(mine_ref.at[source], held_ref.at[source], held_sem.at[source]).wait()
    above = jnp.concatenate([sums_ref[0, source] for source in range(bands)], axis=1).astype(jnp.float32)
    above = jnp.where(core == 1, above, 0.0)
    for below in range(groups - 1):
        pieces = []
        for part, (pair_ref, lower_ref) in enumerate(zip(pair_refs, lower_refs)):

            @pl.when(below < group)
            def _():
                pltpu.make_async_copy(pair_ref, lower_ref.at[below], lower_sem.at[part, below]).wait()

            @pl.when(below >= group)
            def _():
                lower_ref[below] = jnp.zeros(lower_ref.shape[1:], jnp.bfloat16)

            piece = lower_ref[below].astype(jnp.float32)
            size = piece.shape[1] // bands
            pieces.append([piece[:, source * size : (source + 1) * size] for source in range(bands)])
        above = above + jnp.concatenate([piece[source] for source in range(bands) for piece in pieces], axis=1)
    scaled = [
        above[side * pairs : (side + 1) * pairs] * coef_ref[level]
        for side in range(2)
        for level in range(levels)
    ]
    value = jnp.concatenate([held_ref[source] for source in range(bands)], axis=1).astype(jnp.float32)
    value = value + jnp.concatenate(scaled, axis=0)
    same, other = value * stay, swap_pairs(value) * move
    far, near = same + other, same - other
    faces = [value] + [value * sign for sign in signs]
    faces += [far, near * signs[0], far * signs[1], near * signs[2]]
    faces = jnp.concatenate([face.astype(jnp.bfloat16) for face in faces], axis=0)
    grid = lax.dot_general(faces, table_ref[...], TO_LANES, preferred_element_type=jnp.float32)
    forcing = (gain_ref[...] * grid).astype(jnp.bfloat16)
    back = jnp.dot(forcing, table_ref[...], preferred_element_type=jnp.float32)
    back = [back[face * rows : (face + 1) * rows] for face in range(2 * NBLK)]
    total = back[0] + back[1] * signs[0] + back[2] * signs[1] + back[3] * signs[2]
    even = back[4] + back[6] * signs[1]
    odd = back[5] * signs[0] + back[7] * signs[2]
    total = total + (even + odd) * stay + swap_pairs(even - odd) * move
    total = total * scale
    half = rows // 2
    both = jnp.concatenate([total[:half] + total[half:], total[:half] - total[half:]], axis=0)
    both = both.astype(jnp.bfloat16)
    for target in range(bands):
        back_ref[target] = both[:, target * width : (target + 1) * width]
    returns = [
        pltpu.make_async_remote_copy(
            src_ref=back_ref.at[there(ahead)],
            dst_ref=out_ref.at[band],
            send_sem=back_send.at[ahead],
            recv_sem=back_sem.at[band],
            device_id={"band": there(ahead), "lev": lev},
            device_id_type=MESH,
        )
        for ahead in range(1, bands)
    ]
    for copy in returns:
        copy.start()
    pltpu.make_async_copy(back_ref.at[band], out_ref.at[band], back_sem.at[band]).start()
    for source in range(bands):
        pltpu.make_async_copy(back_ref.at[source], out_ref.at[source], back_sem.at[source]).wait()
    for copy in sends + returns:
        copy.wait_send()
    for part in range(len(parts)):
        for copy in totals_out(part):
            copy.wait_send()
        for ahead, copy in enumerate(upper_out(part), 1):

            @pl.when(group + ahead < groups)
            def _():
                copy.wait_send()


def grid_call(adj_spec, legendre, wave_of_slot, traj, lat_weight, traj_exp, traj_order, lev_coef):
    levels, slots, _, degrees = adj_spec.shape
    heights = legendre.shape[1]
    step, sub = slot_step(slots, heights)
    lat_rows, lon_count = traj.shape[1:]
    bands = lax.axis_size("band")
    groups = lax.axis_size("lev") // 2
    pairs = lat_rows // 2
    rows = levels * lat_rows
    mine = (bands, rows, slots * 2)
    total = (bands, lat_rows, slots * 2)
    count = bands * slots * 2
    half = lon_count // (2 * NBLK)
    padded = -(-half // 16) * 16
    chunks = slots // step
    sizes = [part.stop - part.start for part in total_parts(slots, heights)]
    scale = 1.0 / math.sqrt(count // 2)
    dma = pltpu.SemaphoreType.DMA
    bf16 = jnp.bfloat16
    operands = (adj_spec, legendre, wave_of_slot, traj, lat_weight, traj_exp, traj_order, lev_coef)
    return pl.pallas_call(
        functools.partial(grid_kernel, (levels, pairs, scale)),
        in_specs=[LOOSE] * 8,
        out_specs=(VMEM,) * 4,
        out_shape=(
            pltpu.VMEM(mine, bf16),
            pltpu.VMEM(legendre.shape, bf16),
            pltpu.VMEM((slots // sub, sub * heights, LANES), jnp.int16),
            pltpu.VMEM((2, slots * 2), jnp.float32),
        ),
        scratch_shapes=[
            pltpu.VMEM(adj_spec.shape, bf16),
            pltpu.VMEM((2, step // sub, levels * sub * 2, 2 * sub * heights), bf16),
            pltpu.VMEM(mine, bf16),
            pltpu.VMEM(total, bf16),
            pltpu.VMEM(wave_of_slot.shape, jnp.int32),
            pltpu.VMEM(traj.shape, bf16),
            pltpu.SMEM(wave_of_slot.shape, jnp.int32),
            pltpu.SMEM(lat_weight.shape, jnp.float32),
            pltpu.SMEM(traj_exp.shape, jnp.int32),
            pltpu.SMEM(traj_order.shape, jnp.int32),
            pltpu.SMEM(lev_coef.shape, jnp.float32),
            pltpu.VMEM(mine, bf16),
            pltpu.VMEM((2,) + total, bf16),
            [pltpu.VMEM((lat_rows, bands * size), bf16) for size in sizes],
            [pltpu.VMEM((groups, lat_rows, bands * size), bf16) for size in sizes],
            pltpu.VMEM(mine, bf16),
            pltpu.VMEM((1, count), jnp.float32),
            pltpu.VMEM((padded, count), bf16),
            pltpu.VMEM((2 * NBLK * rows, padded), jnp.float32),
            dma((chunks,)),
            dma((chunks,)),
            dma((7,)),
            dma((bands,)),
            dma((bands,)),
            dma((len(sizes), 2, bands)),
            dma((len(sizes), 2, bands)),
            dma((len(sizes), groups)),
            dma((len(sizes), groups)),
            dma((bands,)),
            dma((bands,)),
        ],
        name="grid",
        compiler_params=pltpu.CompilerParams(collective_id=0, has_side_effects=True, vmem_limit_bytes=24 * MIB),
    )(*[in_hbm(value) for value in operands])


def body(adj_spec, wave_of_slot, legendre, lat_weight, traj, traj_exp, traj_order, lev_coef):
    coef, leg, limit, turn = grid_call(
        adj_spec, legendre, wave_of_slot, traj, lat_weight, traj_exp, traj_order, lev_coef
    )
    return analysis_call(coef, leg, limit, turn, adj_spec.shape)


def solution(mesh):
    placed = (
        P("lev", "band", None, None),
        P(),
        P("band", None, None),
        P(),
        P("lev", "band", None),
        P("lev", "band", None),
        P("lev", None),
        P("lev"),
    )
    return jax.shard_map(
        body, mesh=mesh, in_specs=placed, out_specs=P("lev", "band", None, None), check_vma=False
    )
```

```python
import functools
import math

import jax
import jax.numpy as jnp
from jax import lax
from jax.experimental import pallas as pl
from jax.experimental.pallas import tpu as pltpu
from jax.sharding import PartitionSpec as P

NBLK = 4
LANES = 128
MESH = pl.DeviceIdType.MESH
MIB = 1024 * 1024
TO_LANES = (((1,), (1,)), ((), ()))
VMEM = pl.BlockSpec(memory_space=pltpu.VMEM)
SMEM = pl.BlockSpec(memory_space=pltpu.SMEM)
LOOSE = pl.BlockSpec(memory_space=pl.ANY)


def in_hbm(value):
    return pltpu.with_memory_space_constraint(value, pltpu.HBM)


def slot_step(slots, heights):
    step = 64 if slots % 64 == 0 else slots
    sub = max(1, 256 // (2 * heights))
    while step % sub:
        sub -= 1
    return step, sub


def iota(shape, dim):
    return lax.broadcasted_iota(jnp.int32, shape, dim)


def swap_pairs(value):
    lane = iota(value.shape, 1)
    width = value.shape[1]
    return jnp.where(lane % 2 == 0, pltpu.roll(value, width - 1, 1), pltpu.roll(value, 1, 1))


def cos_turn(count, period):
    left = count - jnp.floor(count * (1.0 / period)) * period
    angle = math.pi * (0.5 - jnp.abs(left * (2.0 / period) - 1.0))
    square = angle * angle
    series = 1.0
    for order in (11, 9, 7, 5, 3):
        series = 1.0 - series * square * (1.0 / (order * (order - 1)))
    return -angle * series


def own_group(levels, sub, heights):
    shape = (levels * sub * 2, 2 * sub * heights)
    row, lane = iota(shape, 0), iota(shape, 1)
    return (row % (sub * 2)) // 2 == (lane % (sub * heights)) // heights


def chunk_lanes(index, step, slots):
    if step == slots:
        return slice(None)
    return pl.ds(pl.multiple_of(index * (step * 2), step * 2), step * 2)


def half_turn(waves_ref, first, step, lon_count):
    shape = (8, step * 2)
    slot = iota(shape, 1) // 2
    parts = []
    for begin in range(0, step, 8):
        wave = jnp.zeros(shape, jnp.int32)
        for s in range(begin, min(begin + 8, step)):
            wave = jnp.where(slot == s, waves_ref[first + s], wave)
        parts.append(wave)
    wave = sum(parts).astype(jnp.float32)[:1]
    sign = 1.0 - 2.0 * (iota((1, step * 2), 1) % 2).astype(jnp.float32)
    period = 2 * lon_count
    return cos_turn(wave, period), cos_turn(wave + 1.5 * lon_count, period) * sign


def masked_table(leg, limit):
    rows, degrees = leg.shape
    lane = iota((rows, LANES), 1)
    even = (lane % 2 == 0).astype(jnp.int16) == 1
    lane = lane.astype(jnp.int16)
    zero = jnp.zeros((rows, LANES), jnp.bfloat16)
    tiles = []
    for tile in range(0, degrees, LANES):
        part = jnp.where(lane + jnp.int16(tile) < limit, leg[:, tile : tile + LANES], zero)
        tiles.append(jnp.concatenate([jnp.where(even, part, zero), jnp.where(even, zero, part)], axis=0))
    return jnp.concatenate(tiles, axis=1)


def synthesize(
    lon_count, out_ref, total_ref, leg_ref, limit_ref, turn_ref, x_ref, kept_ref, waves_ref, weight_ref, coef_ref, start, arrive, first, early
):
    levels, slots, _, degrees = x_ref.shape
    heights = leg_ref.shape[1]
    step, sub = slot_step(slots, heights)
    bands = out_ref.shape[0]
    pairs = heights // bands
    chunks = slots // step
    begin = lax.axis_index("band") * slots
    depth = min(2, chunks)
    for index in range(depth):
        start(index)
    first()

    keep = own_group(levels, sub, heights)
    fold = (2 * heights, 2 * sub * heights)
    side, parity = iota(fold, 0) // heights, iota(fold, 1) // (sub * heights)
    sign = jnp.where(side * parity == 1, -1.0, 1.0)
    fold = jnp.where(iota(fold, 0) % heights == iota(fold, 1) % heights, sign, 0.0).astype(jnp.bfloat16)
    row = iota((2 * heights, 1), 0) % heights
    weight = jnp.zeros((2 * heights, 1), jnp.float32)
    for h in range(heights):
        weight = jnp.where(row == h, weight_ref[h], weight)

    def prepare(index, carry):
        lanes = chunk_lanes(index, step, slots)
        turn_cos, turn_sin = half_turn(waves_ref, begin + index * step, step, lon_count)
        turn_ref[0:1, lanes] = turn_cos
        turn_ref[1:2, lanes] = turn_sin
        for first in range(0, step, sub):
            here = begin + index * step + first
            limit = [jnp.full((heights, LANES), degrees - waves_ref[here + s], jnp.int32) for s in range(sub)]
            limit_ref[(index * step + first) // sub] = jnp.concatenate(limit, axis=0).astype(jnp.int16)
        return carry

    lax.fori_loop(0, chunks, prepare, 0)

    def multiply(index):
        for number, first in enumerate(range(0, step, sub)):
            local = pl.ds(index * step + first, sub)
            table = masked_table(
                leg_ref[local].reshape(sub * heights, degrees), limit_ref[(index * step + first) // sub]
            )
            spec = x_ref[:, local].reshape(levels * sub * 2, degrees)
            cross = lax.dot_general(spec, table, TO_LANES, preferred_element_type=jnp.float32)
            kept_ref[lax.rem(index, 2), number] = jnp.where(keep, cross, 0.0).astype(jnp.bfloat16)

    def finish(index):
        lanes = chunk_lanes(index, step, slots)
        turn_cos, turn_sin = turn_ref[0:1, lanes], turn_ref[1:2, lanes]
        total = None
        for level in range(levels + 1):
            if level < levels:
                rows = slice(level * sub * 2, (level + 1) * sub * 2)
                value = kept_ref[lax.rem(index, 2), :, rows].reshape(step * 2, 2 * sub * heights)
                value = lax.dot_general(fold, value, TO_LANES, preferred_element_type=jnp.float32) * weight
                value = value * turn_cos + swap_pairs(value) * turn_sin
                held = value if total is None else value + coef_ref[level] * total
                total = value if total is None else total + value
                base, ref = level * pairs, out_ref
            else:
                held, base, ref = total, 0, total_ref
            sent = held.astype(jnp.bfloat16)
            half = ref.shape[1] // 2
            for side in range(2):
                for band in range(bands):
                    first = side * heights + band * pairs
                    start = side * half + base
                    ref[band, start : start + pairs, lanes] = sent[first : first + pairs]

    def take(index):
        arrive(index)

        @pl.when(index + depth < chunks)
        def _():
            start(index + depth)

    take(0)
    multiply(0)

    def chunk(index, carry):
        take(index)
        finish(index - 1)
        multiply(index)
        return carry

    if chunks > 2:
        lax.fori_loop(1, chunks - 1, chunk, 0)
        early()
        chunk(chunks - 1, 0)
    else:
        lax.fori_loop(1, chunks, chunk, 0)
    finish(chunks - 1)


def total_parts(slots, heights):
    step, _ = slot_step(slots, heights)
    chunks = slots // step
    ends = [0, (chunks - 2) * step * 2, slots * 2] if chunks > 2 else [0, slots * 2]
    return [slice(*pair) for pair in zip(ends, ends[1:])]


def analysis_kernel(coef_ref, leg_ref, limit_ref, turn_ref, out_hbm, out_ref, part_ref, out_sem):
    levels, slots, _, degrees = out_hbm.shape
    bands = coef_ref.shape[0]
    heights = leg_ref.shape[1]
    pairs = heights // bands
    step, sub = slot_step(slots, heights)
    chunks = slots // step
    keep = own_group(levels, sub, heights)
    tile = (2 * heights, 2 * sub * heights)
    row, lane = iota(tile, 0), iota(tile, 1)
    same = (row % heights == lane % heights) & (row // heights == lane // (sub * heights))
    tile = jnp.where(same, 1.0, 0.0).astype(jnp.bfloat16)

    def copy(index):
        part = pl.ds(index * step, step)
        return pltpu.make_async_copy(out_ref.at[:, part], out_hbm.at[:, part], out_sem.at[index])

    def prepare(index):
        lanes = chunk_lanes(index, step, slots)
        turn_cos, turn_sin = turn_ref[0:1, lanes], turn_ref[1:2, lanes]
        held = coef_ref[:, :, lanes].astype(jnp.float32)
        spread = []
        for level in range(levels):
            value = []
            for side in range(2):
                for band in range(bands):
                    first = (side * levels + level) * pairs
                    value.append(held[band, first : first + pairs])
            value = jnp.concatenate(value, axis=0)
            value = (value * turn_cos - swap_pairs(value) * turn_sin).astype(jnp.bfloat16)
            spread.append(
                lax.dot_general(value, tile, (((0,), (0,)), ((), ())), preferred_element_type=jnp.float32)
            )
        for number, first in enumerate(range(0, step, sub)):
            rows = slice(first * 2, (first + sub) * 2)
            part = jnp.concatenate([value[rows] for value in spread], axis=0)
            part_ref[lax.rem(index, 2), number] = jnp.where(keep, part, 0.0).astype(jnp.bfloat16)

    def multiply(index):
        for number, first in enumerate(range(0, step, sub)):
            local = pl.ds(index * step + first, sub)
            table = masked_table(
                leg_ref[local].reshape(sub * heights, degrees), limit_ref[(index * step + first) // sub]
            )
            total = jnp.dot(part_ref[lax.rem(index, 2), number], table, preferred_element_type=jnp.float32)
            out_ref[:, local] = total.astype(jnp.bfloat16).reshape(levels, sub, 2, degrees)

    prepare(0)

    def chunk(index, carry):
        multiply(index)
        prepare(index + 1)
        copy(index).start()
        return carry

    lax.fori_loop(0, chunks - 1, chunk, 0)
    multiply(chunks - 1)
    copy(chunks - 1).start()
    for index in range(chunks):
        copy(index).wait()


def analysis_call(coef, leg, limit, turn, shape):
    levels, slots, _, degrees = shape
    heights = leg.shape[1]
    step, sub = slot_step(slots, heights)
    return pl.pallas_call(
        analysis_kernel,
        in_specs=[VMEM] * 4,
        out_specs=LOOSE,
        out_shape=pltpu.HBM(shape, jnp.bfloat16),
        scratch_shapes=[
            pltpu.VMEM(shape, jnp.bfloat16),
            pltpu.VMEM((2, step // sub, levels * sub * 2, 2 * sub * heights), jnp.bfloat16),
            pltpu.SemaphoreType.DMA((slots // step,)),
        ],
        name="analysis",
        compiler_params=pltpu.CompilerParams(vmem_limit_bytes=20 * MIB),
    )(coef, leg, limit, turn)


def fill_table(waves_ref, table_ref, lon_count):
    period = 2 * lon_count
    rows = table_ref.shape[0]
    back = 1.5 * lon_count
    row = lax.broadcasted_iota(jnp.int32, (8, LANES), 0).astype(jnp.float32)
    part = lax.broadcasted_iota(jnp.int32, (8, LANES), 1) % 2
    shift = part.astype(jnp.float32) * (lon_count // 2)

    def column(index, carry):
        lanes = pl.ds(pl.multiple_of(index * LANES, LANES), LANES)
        wave = jnp.broadcast_to(waves_ref[0:1, lanes], (8, LANES))
        near = wave * (2.0 * row + 1.0)
        near_cos, near_sin = cos_turn(near, period), cos_turn(near + back, period)
        middle = wave * (16.0 * row)
        middle_cos, middle_sin = cos_turn(middle, period), cos_turn(middle + back, period)
        fine = []
        for j in range(8):
            c, s = middle_cos[j : j + 1], middle_sin[j : j + 1]
            fine.append((near_cos * c - near_sin * s, near_sin * c + near_cos * s))
        for group in range(-(-rows // 512)):
            far = wave * (128.0 * (row + 8.0 * group)) + shift
            far_cos, far_sin = cos_turn(far, period), cos_turn(far + back, period)
            for n in range(8):
                c, s = far_cos[n : n + 1], far_sin[n : n + 1]
                for j in range(0, 8, 2):
                    first = (group * 8 + n) * 64 + j * 8
                    if first < rows:
                        block = [fine[i][0] * c - fine[i][1] * s for i in (j, j + 1)]
                        table_ref[first : first + 16, lanes] = jnp.concatenate(block).astype(jnp.bfloat16)
        return carry

    lax.fori_loop(0, table_ref.shape[1] // LANES, column, 0)


def fill_waves(order_ref, waves_ref):
    wave = order_ref[...].astype(jnp.float32).reshape(order_ref.shape[0] // LANES, LANES)
    high = jnp.floor(wave * (1.0 / 256.0))
    digits = (high.astype(jnp.bfloat16), (wave - 256.0 * high).astype(jnp.bfloat16))
    for half in range(2):
        source = iota((LANES, LANES), 1) // 2 + half * (LANES // 2)
        twice = jnp.where(iota((LANES, LANES), 0) == source, 1.0, 0.0).astype(jnp.bfloat16)
        high, low = [jnp.dot(digit, twice, preferred_element_type=jnp.float32) for digit in digits]
        value = high * 256.0 + low
        for r in range(wave.shape[0]):
            first = (2 * r + half) * LANES
            waves_ref[0:1, first : first + LANES] = value[r : r + 1]


def fill_gain(traj_ref, exp_ref, order_ref, gain_ref, scale):
    levels, lat_rows, lon_count = traj_ref.shape
    quarter = lon_count // NBLK
    half = quarter // 2
    rows = levels * lat_rows
    pairs = lat_rows // 2
    padded = gain_ref.shape[1]
    stored = jnp.concatenate([traj_ref[r].astype(jnp.float32) for r in range(levels)], axis=0)
    stored = stored.astype(jnp.bfloat16)
    turned = iota((LANES, LANES), 0) + iota((LANES, LANES), 1) == LANES - 1
    turned = jnp.where(turned, 1.0, 0.0).astype(jnp.bfloat16)
    row, column = iota((rows, rows), 0), iota((rows, rows), 1)
    held = jnp.zeros((rows, rows), jnp.int32)
    for r in range(levels):
        held = jnp.where(column // lat_rows == r, order_ref[0, r], held)
    lat = 2 * (row % pairs) + row // (levels * pairs)
    hit = (held == row // pairs % levels) & (column % lat_rows == lat)
    for block in range(NBLK):
        power = jnp.zeros((rows, rows), jnp.int32)
        for r in range(levels):
            for q in range(lat_rows):
                power = jnp.where(column == r * lat_rows + q, exp_ref[r, q, block], power)
        factor = jnp.where(power < 0, jnp.where(power == -1, 0.5, 0.25), jnp.where(power == 0, 1.0, 2.0))
        factor = jnp.where(power == 2, 4.0, factor)
        pick = jnp.where(hit, factor, 0.0).astype(jnp.bfloat16)
        for reverse in range(2):
            if reverse:
                last = (block + 1) * quarter - 1
                stop = last // LANES + 1
                skip = stop * LANES - 1 - last
                tiles = -(-(skip + half) // LANES)
                tile = stop - tiles
            else:
                tile = block * quarter // LANES
                skip = block * quarter - tile * LANES
                tiles = -(-(skip + half) // LANES)
                stop = tile + tiles
            window = stored[:, tile * LANES : min(stop * LANES, lon_count)]
            if stop * LANES > lon_count:
                fill = jnp.zeros((rows, stop * LANES - lon_count), jnp.bfloat16)
                window = jnp.concatenate([window, fill], axis=1)
            value = jnp.dot(pick, window, preferred_element_type=jnp.float32)
            if reverse:
                value = value.astype(jnp.bfloat16)
                stack = [value[:, t * LANES : (t + 1) * LANES] for t in reversed(range(tiles))]
                value = jnp.dot(jnp.concatenate(stack, axis=0), turned, preferred_element_type=jnp.float32)
                value = jnp.concatenate([value[t * rows : (t + 1) * rows] for t in range(tiles)], axis=1)
            value = (1.0 + jnp.tanh(value[:, skip : skip + half])) * scale
            face = block + (NBLK if (block + reverse) % 2 else 0)
            value = jnp.concatenate([value, jnp.zeros((rows, padded - half), jnp.float32)], axis=1)
            gain_ref[face * rows : (face + 1) * rows] = value


def grid_kernel(
    sizes,
    x_hbm,
    leg_hbm,
    wave_hbm,
    traj_hbm,
    weight_hbm,
    exp_hbm,
    order_hbm,
    coef_hbm,
    out_ref,
    leg_ref,
    limit_ref,
    turn_ref,
    x_ref,
    kept_ref,
    mine_ref,
    total_ref,
    wave_of_ref,
    traj_ref,
    slot_ref,
    weight_ref,
    exp_ref,
    order_ref,
    coef_ref,
    held_ref,
    sums_ref,
    pair_refs,
    lower_refs,
    back_ref,
    waves_ref,
    table_ref,
    gain_ref,
    x_sem,
    leg_sem,
    small_sem,
    mine_sem,
    held_sem,
    sums_send,
    sums_sem,
    pair_send,
    lower_sem,
    back_send,
    back_sem,
):
    levels, pairs, scale = sizes
    bands, rows, width = mine_ref.shape
    lon_count = traj_ref.shape[2]
    groups = lower_refs[0].shape[0]
    parts = total_parts(x_ref.shape[1], leg_ref.shape[1])
    band, lev = lax.axis_index("band"), lax.axis_index("lev")
    group, core = lev // 2, lev % 2

    def there(ahead):
        return lax.rem(band + ahead, bands)

    barrier = pltpu.get_barrier_semaphore()
    small = ((wave_hbm, slot_ref), (weight_hbm, weight_ref), (coef_hbm, coef_ref), (wave_hbm, wave_of_ref))
    small += ((traj_hbm, traj_ref), (exp_hbm, exp_ref), (order_hbm, order_ref))
    small = [pltpu.make_async_copy(source, ref, small_sem.at[n]) for n, (source, ref) in enumerate(small)]
    for copy in small:
        copy.start()
    step, _ = slot_step(x_ref.shape[1], leg_ref.shape[1])

    def copies(index):
        part = pl.ds(index * step, step)
        return (
            pltpu.make_async_copy(x_hbm.at[:, part], x_ref.at[:, part], x_sem.at[index]),
            pltpu.make_async_copy(leg_hbm.at[part], leg_ref.at[part], leg_sem.at[index]),
        )

    def start(index):
        for copy in copies(index):
            copy.start()

    def arrive(index):
        for copy in copies(index):
            copy.wait()

    def shadow():
        for copy in small[3:]:
            copy.wait()
        fill_gain(traj_ref, exp_ref, order_ref, gain_ref, scale)
        fill_waves(wave_of_ref, waves_ref)

    def first():
        for ahead in range(bands):
            for side in range(2):
                if ahead or side:
                    pl.semaphore_signal(
                        barrier,
                        inc=1,
                        device_id={"band": there(ahead), "lev": group * 2 + (core + side) % 2},
                        device_id_type=MESH,
                    )
        for ahead in range(1, groups):
            pl.semaphore_signal(
                barrier,
                inc=1,
                device_id={"band": band, "lev": lax.rem(group + ahead, groups) * 2 + core},
                device_id_type=MESH,
            )
        for copy in small[:3]:
            copy.wait()

    def totals_out(part):
        lanes = parts[part]
        return [
            pltpu.make_async_remote_copy(
                src_ref=total_ref.at[there(ahead), :, lanes],
                dst_ref=sums_ref.at[core, band, :, lanes],
                send_sem=sums_send.at[part, side, ahead],
                recv_sem=sums_sem.at[part, core, band],
                device_id={"band": there(ahead), "lev": group * 2 + (core + side) % 2},
                device_id_type=MESH,
            )
            for ahead in range(bands)
            for side in range(2)
            if ahead or side
        ]

    def send_totals(part):
        lanes = parts[part]
        for copy in totals_out(part):
            copy.start()
        pltpu.make_async_copy(
            total_ref.at[band, :, lanes], sums_ref.at[core, band, :, lanes], sums_sem.at[part, core, band]
        ).start()

    def upper_out(part):
        return [
            pltpu.make_async_remote_copy(
                src_ref=pair_refs[part],
                dst_ref=lower_refs[part].at[group],
                send_sem=pair_send.at[part, ahead],
                recv_sem=lower_sem.at[part, group],
                device_id={"band": band, "lev": jnp.minimum(group + ahead, groups - 1) * 2 + core},
                device_id_type=MESH,
            )
            for ahead in range(1, groups)
        ]

    def pass_up(part):
        lanes = parts[part]
        for source in range(bands):
            for side in range(2):
                pltpu.make_async_copy(
                    total_ref.at[source, :, lanes], sums_ref.at[side, source, :, lanes], sums_sem.at[part, side, source]
                ).wait()
        pair = []
        for source in range(bands):
            both = [sums_ref[side, source, :, lanes].astype(jnp.float32) for side in range(2)]
            pair.append((both[0] + both[1]).astype(jnp.bfloat16))
        pair_refs[part][...] = jnp.concatenate(pair, axis=1)
        for ahead, copy in enumerate(upper_out(part), 1):

            @pl.when(group + ahead < groups)
            def _():
                copy.start()

    def early():
        pl.semaphore_wait(barrier, 2 * bands - 1 + groups - 1)
        send_totals(0)

    synthesize(
        lon_count,
        mine_ref,
        total_ref,
        leg_ref,
        limit_ref,
        turn_ref,
        x_ref,
        kept_ref,
        slot_ref,
        weight_ref,
        coef_ref,
        start,
        arrive,
        first,
        early,
    )
    if len(parts) == 1:
        early()
    else:
        send_totals(1)
    sends = [
        pltpu.make_async_remote_copy(
            src_ref=mine_ref.at[there(ahead)],
            dst_ref=held_ref.at[band],
            send_sem=mine_sem.at[ahead],
            recv_sem=held_sem.at[band],
            device_id={"band": there(ahead), "lev": lev},
            device_id_type=MESH,
        )
        for ahead in range(1, bands)
    ]
    for copy in sends:
        copy.start()
    pltpu.make_async_copy(mine_ref.at[band], held_ref.at[band], held_sem.at[band]).start()
    if len(parts) > 1:
        pass_up(0)
    shadow()
    pass_up(len(parts) - 1)

    fill_table(waves_ref, table_ref, lon_count)

    wave = waves_ref[...]
    part = iota(wave.shape, 1) % 2
    sign_c = 1.0 - 2.0 * part.astype(jnp.float32)
    sign_m = 1.0 - 2.0 * (wave - 2.0 * jnp.floor(wave * 0.5))
    phase = wave - 4.0 * jnp.floor(wave * 0.25)
    stay = jnp.where(phase == 0.0, sign_c, jnp.where(phase == 2.0, -sign_c, 0.0))
    move = jnp.where(phase == 1.0, -1.0, jnp.where(phase == 3.0, 1.0, 0.0))
    signs = (sign_m * sign_c, sign_m, sign_c)

    for source in range(bands):
        pltpu.make_async_copy(mine_ref.at[source], held_ref.at[source], held_sem.at[source]).wait()
    above = jnp.concatenate([sums_ref[0, source] for source in range(bands)], axis=1).astype(jnp.float32)
    above = jnp.where(core == 1, above, 0.0)
    for below in range(groups - 1):
        pieces = []
        for part, (pair_ref, lower_ref) in enumerate(zip(pair_refs, lower_refs)):

            @pl.when(below < group)
            def _():
                pltpu.make_async_copy(pair_ref, lower_ref.at[below], lower_sem.at[part, below]).wait()

            @pl.when(below >= group)
            def _():
                lower_ref[below] = jnp.zeros(lower_ref.shape[1:], jnp.bfloat16)

            piece = lower_ref[below].astype(jnp.float32)
            size = piece.shape[1] // bands
            pieces.append([piece[:, source * size : (source + 1) * size] for source in range(bands)])
        above = above + jnp.concatenate([piece[source] for source in range(bands) for piece in pieces], axis=1)
    scaled = [
        above[side * pairs : (side + 1) * pairs] * coef_ref[level]
        for side in range(2)
        for level in range(levels)
    ]
    value = jnp.concatenate([held_ref[source] for source in range(bands)], axis=1).astype(jnp.float32)
    value = value + jnp.concatenate(scaled, axis=0)
    same, other = value * stay, swap_pairs(value) * move
    far, near = same + other, same - other
    faces = [value] + [value * sign for sign in signs]
    faces += [far, near * signs[0], far * signs[1], near * signs[2]]
    faces = jnp.concatenate([face.astype(jnp.bfloat16) for face in faces], axis=0)
    grid = lax.dot_general(faces, table_ref[...], TO_LANES, preferred_element_type=jnp.float32)
    forcing = (gain_ref[...] * grid).astype(jnp.bfloat16)
    back = jnp.dot(forcing, table_ref[...], preferred_element_type=jnp.float32)
    back = [back[face * rows : (face + 1) * rows] for face in range(2 * NBLK)]
    total = back[0] + back[1] * signs[0] + back[2] * signs[1] + back[3] * signs[2]
    even = back[4] + back[6] * signs[1]
    odd = back[5] * signs[0] + back[7] * signs[2]
    total = total + (even + odd) * stay + swap_pairs(even - odd) * move
    total = total * scale
    half = rows // 2
    both = jnp.concatenate([total[:half] + total[half:], total[:half] - total[half:]], axis=0)
    both = both.astype(jnp.bfloat16)
    for target in range(bands):
        back_ref[target] = both[:, target * width : (target + 1) * width]
    returns = [
        pltpu.make_async_remote_copy(
            src_ref=back_ref.at[there(ahead)],
            dst_ref=out_ref.at[band],
            send_sem=back_send.at[ahead],
            recv_sem=back_sem.at[band],
            device_id={"band": there(ahead), "lev": lev},
            device_id_type=MESH,
        )
        for ahead in range(1, bands)
    ]
    for copy in returns:
        copy.start()
    pltpu.make_async_copy(back_ref.at[band], out_ref.at[band], back_sem.at[band]).start()
    for source in range(bands):
        pltpu.make_async_copy(back_ref.at[source], out_ref.at[source], back_sem.at[source]).wait()
    for copy in sends + returns:
        copy.wait_send()
    for part in range(len(parts)):
        for copy in totals_out(part):
            copy.wait_send()
        for ahead, copy in enumerate(upper_out(part), 1):

            @pl.when(group + ahead < groups)
            def _():
                copy.wait_send()


def grid_call(adj_spec, legendre, wave_of_slot, traj, lat_weight, traj_exp, traj_order, lev_coef):
    levels, slots, _, degrees = adj_spec.shape
    heights = legendre.shape[1]
    step, sub = slot_step(slots, heights)
    lat_rows, lon_count = traj.shape[1:]
    bands = lax.axis_size("band")
    groups = lax.axis_size("lev") // 2
    pairs = lat_rows // 2
    rows = levels * lat_rows
    mine = (bands, rows, slots * 2)
    total = (bands, lat_rows, slots * 2)
    count = bands * slots * 2
    half = lon_count // (2 * NBLK)
    padded = -(-half // 16) * 16
    chunks = slots // step
    sizes = [part.stop - part.start for part in total_parts(slots, heights)]
    scale = 1.0 / math.sqrt(count // 2)
    dma = pltpu.SemaphoreType.DMA
    bf16 = jnp.bfloat16
    operands = (adj_spec, legendre, wave_of_slot, traj, lat_weight, traj_exp, traj_order, lev_coef)
    return pl.pallas_call(
        functools.partial(grid_kernel, (levels, pairs, scale)),
        in_specs=[LOOSE] * 8,
        out_specs=(VMEM,) * 4,
        out_shape=(
            pltpu.VMEM(mine, bf16),
            pltpu.VMEM(legendre.shape, bf16),
            pltpu.VMEM((slots // sub, sub * heights, LANES), jnp.int16),
            pltpu.VMEM((2, slots * 2), jnp.float32),
        ),
        scratch_shapes=[
            pltpu.VMEM(adj_spec.shape, bf16),
            pltpu.VMEM((2, step // sub, levels * sub * 2, 2 * sub * heights), bf16),
            pltpu.VMEM(mine, bf16),
            pltpu.VMEM(total, bf16),
            pltpu.VMEM(wave_of_slot.shape, jnp.int32),
            pltpu.VMEM(traj.shape, bf16),
            pltpu.SMEM(wave_of_slot.shape, jnp.int32),
            pltpu.SMEM(lat_weight.shape, jnp.float32),
            pltpu.SMEM(traj_exp.shape, jnp.int32),
            pltpu.SMEM(traj_order.shape, jnp.int32),
            pltpu.SMEM(lev_coef.shape, jnp.float32),
            pltpu.VMEM(mine, bf16),
            pltpu.VMEM((2,) + total, bf16),
            [pltpu.VMEM((lat_rows, bands * size), bf16) for size in sizes],
            [pltpu.VMEM((groups, lat_rows, bands * size), bf16) for size in sizes],
            pltpu.VMEM(mine, bf16),
            pltpu.VMEM((1, count), jnp.float32),
            pltpu.VMEM((padded, count), bf16),
            pltpu.VMEM((2 * NBLK * rows, padded), jnp.float32),
            dma((chunks,)),
            dma((chunks,)),
            dma((7,)),
            dma((bands,)),
            dma((bands,)),
            dma((len(sizes), 2, bands)),
            dma((len(sizes), 2, bands)),
            dma((len(sizes), groups)),
            dma((len(sizes), groups)),
            dma((bands,)),
            dma((bands,)),
        ],
        name="grid",
        compiler_params=pltpu.CompilerParams(collective_id=0, has_side_effects=True, vmem_limit_bytes=24 * MIB),
    )(*[in_hbm(value) for value in operands])


def body(adj_spec, wave_of_slot, legendre, lat_weight, traj, traj_exp, traj_order, lev_coef):
    coef, leg, limit, turn = grid_call(
        adj_spec, legendre, wave_of_slot, traj, lat_weight, traj_exp, traj_order, lev_coef
    )
    return analysis_call(coef, leg, limit, turn, adj_spec.shape)


def solution(mesh):
    placed = (
        P("lev", "band", None, None),
        P(),
        P("band", None, None),
        P(),
        P("lev", "band", None),
        P("lev", "band", None),
        P("lev", None),
        P("lev"),
    )
    return jax.shard_map(
        body, mesh=mesh, in_specs=placed, out_specs=P("lev", "band", None, None), check_vma=False
    )
```

```python
import functools
import math

import jax
import jax.numpy as jnp
from jax import lax
from jax.experimental import pallas as pl
from jax.experimental.pallas import tpu as pltpu
from jax.sharding import PartitionSpec as P

NBLK = 4
LANES = 128
MESH = pl.DeviceIdType.MESH
MIB = 1024 * 1024
TO_LANES = (((1,), (1,)), ((), ()))
VMEM = pl.BlockSpec(memory_space=pltpu.VMEM)
SMEM = pl.BlockSpec(memory_space=pltpu.SMEM)
LOOSE = pl.BlockSpec(memory_space=pl.ANY)


def in_hbm(value):
    return pltpu.with_memory_space_constraint(value, pltpu.HBM)


def slot_step(slots, heights):
    step = 64 if slots % 64 == 0 else slots
    sub = max(1, 256 // (2 * heights))
    while step % sub:
        sub -= 1
    return step, sub


def iota(shape, dim):
    return lax.broadcasted_iota(jnp.int32, shape, dim)


def swap_pairs(value):
    lane = iota(value.shape, 1)
    width = value.shape[1]
    return jnp.where(lane % 2 == 0, pltpu.roll(value, width - 1, 1), pltpu.roll(value, 1, 1))


def cos_turn(count, period):
    left = count - jnp.floor(count * (1.0 / period)) * period
    angle = math.pi * (0.5 - jnp.abs(left * (2.0 / period) - 1.0))
    square = angle * angle
    series = 1.0
    for order in (11, 9, 7, 5, 3):
        series = 1.0 - series * square * (1.0 / (order * (order - 1)))
    return -angle * series


def own_group(levels, sub, heights):
    shape = (levels * sub * 2, 2 * sub * heights)
    row, lane = iota(shape, 0), iota(shape, 1)
    return (row % (sub * 2)) // 2 == (lane % (sub * heights)) // heights


def chunk_lanes(index, step, slots):
    if step == slots:
        return slice(None)
    return pl.ds(pl.multiple_of(index * (step * 2), step * 2), step * 2)


def half_turn(waves_ref, first, step, lon_count):
    shape = (8, step * 2)
    slot = iota(shape, 1) // 2
    parts = []
    for begin in range(0, step, 8):
        wave = jnp.zeros(shape, jnp.int32)
        for s in range(begin, min(begin + 8, step)):
            wave = jnp.where(slot == s, waves_ref[first + s], wave)
        parts.append(wave)
    wave = sum(parts).astype(jnp.float32)[:1]
    sign = 1.0 - 2.0 * (iota((1, step * 2), 1) % 2).astype(jnp.float32)
    period = 2 * lon_count
    return cos_turn(wave, period), cos_turn(wave + 1.5 * lon_count, period) * sign


def masked_table(leg, limit):
    rows, degrees = leg.shape
    lane = iota((rows, LANES), 1)
    even = (lane % 2 == 0).astype(jnp.int16) == 1
    lane = lane.astype(jnp.int16)
    zero = jnp.zeros((rows, LANES), jnp.bfloat16)
    tiles = []
    for tile in range(0, degrees, LANES):
        part = jnp.where(lane + jnp.int16(tile) < limit, leg[:, tile : tile + LANES], zero)
        tiles.append(jnp.concatenate([jnp.where(even, part, zero), jnp.where(even, zero, part)], axis=0))
    return jnp.concatenate(tiles, axis=1)


def synthesize(
    lon_count, out_ref, total_ref, leg_ref, limit_ref, turn_ref, x_ref, kept_ref, waves_ref, weight_ref, coef_ref, start, arrive, first, early
):
    levels, slots, _, degrees = x_ref.shape
    heights = leg_ref.shape[1]
    step, sub = slot_step(slots, heights)
    bands = out_ref.shape[0]
    pairs = heights // bands
    chunks = slots // step
    begin = lax.axis_index("band") * slots
    depth = min(2, chunks)
    for index in range(depth):
        start(index)
    first()

    keep = own_group(levels, sub, heights)
    fold = (2 * heights, 2 * sub * heights)
    side, parity = iota(fold, 0) // heights, iota(fold, 1) // (sub * heights)
    sign = jnp.where(side * parity == 1, -1.0, 1.0)
    fold = jnp.where(iota(fold, 0) % heights == iota(fold, 1) % heights, sign, 0.0).astype(jnp.bfloat16)
    row = iota((2 * heights, 1), 0) % heights
    weight = jnp.zeros((2 * heights, 1), jnp.float32)
    for h in range(heights):
        weight = jnp.where(row == h, weight_ref[h], weight)

    def prepare(index, carry):
        lanes = chunk_lanes(index, step, slots)
        turn_cos, turn_sin = half_turn(waves_ref, begin + index * step, step, lon_count)
        turn_ref[0:1, lanes] = turn_cos
        turn_ref[1:2, lanes] = turn_sin
        for first in range(0, step, sub):
            here = begin + index * step + first
            limit = [jnp.full((heights, LANES), degrees - waves_ref[here + s], jnp.int32) for s in range(sub)]
            limit_ref[(index * step + first) // sub] = jnp.concatenate(limit, axis=0).astype(jnp.int16)
        return carry

    lax.fori_loop(0, chunks, prepare, 0)

    def multiply(index):
        for number, first in enumerate(range(0, step, sub)):
            local = pl.ds(index * step + first, sub)
            table = masked_table(
                leg_ref[local].reshape(sub * heights, degrees), limit_ref[(index * step + first) // sub]
            )
            spec = x_ref[:, local].reshape(levels * sub * 2, degrees)
            cross = lax.dot_general(spec, table, TO_LANES, preferred_element_type=jnp.float32)
            kept_ref[lax.rem(index, 2), number] = jnp.where(keep, cross, 0.0).astype(jnp.bfloat16)

    def finish(index):
        lanes = chunk_lanes(index, step, slots)
        turn_cos, turn_sin = turn_ref[0:1, lanes], turn_ref[1:2, lanes]
        total = None
        for level in range(levels + 1):
            if level < levels:
                rows = slice(level * sub * 2, (level + 1) * sub * 2)
                value = kept_ref[lax.rem(index, 2), :, rows].reshape(step * 2, 2 * sub * heights)
                value = lax.dot_general(fold, value, TO_LANES, preferred_element_type=jnp.float32) * weight
                value = value * turn_cos + swap_pairs(value) * turn_sin
                held = value if total is None else value + coef_ref[level] * total
                total = value if total is None else total + value
                base, ref = level * pairs, out_ref
            else:
                held, base, ref = total, 0, total_ref
            sent = held.astype(jnp.bfloat16)
            half = ref.shape[1] // 2
            for side in range(2):
                for band in range(bands):
                    first = side * heights + band * pairs
                    start = side * half + base
                    ref[band, start : start + pairs, lanes] = sent[first : first + pairs]

    def take(index):
        arrive(index)

        @pl.when(index + depth < chunks)
        def _():
            start(index + depth)

    take(0)
    multiply(0)

    def chunk(index, carry):
        take(index)
        finish(index - 1)
        multiply(index)
        return carry

    if chunks > 2:
        lax.fori_loop(1, chunks - 1, chunk, 0)
        early()
        chunk(chunks - 1, 0)
    else:
        lax.fori_loop(1, chunks, chunk, 0)
    finish(chunks - 1)


def total_parts(slots, heights):
    step, _ = slot_step(slots, heights)
    chunks = slots // step
    ends = [0, (chunks - 2) * step * 2, slots * 2] if chunks > 2 else [0, slots * 2]
    return [slice(*pair) for pair in zip(ends, ends[1:])]


def analysis_kernel(coef_ref, leg_ref, limit_ref, turn_ref, out_hbm, out_ref, part_ref, out_sem):
    levels, slots, _, degrees = out_hbm.shape
    bands = coef_ref.shape[0]
    heights = leg_ref.shape[1]
    pairs = heights // bands
    step, sub = slot_step(slots, heights)
    chunks = slots // step
    keep = own_group(levels, sub, heights)
    tile = (2 * heights, 2 * sub * heights)
    row, lane = iota(tile, 0), iota(tile, 1)
    same = (row % heights == lane % heights) & (row // heights == lane // (sub * heights))
    tile = jnp.where(same, 1.0, 0.0).astype(jnp.bfloat16)

    def copy(index):
        part = pl.ds(index * step, step)
        return pltpu.make_async_copy(out_ref.at[:, part], out_hbm.at[:, part], out_sem.at[index])

    def prepare(index):
        lanes = chunk_lanes(index, step, slots)
        turn_cos, turn_sin = turn_ref[0:1, lanes], turn_ref[1:2, lanes]
        held = coef_ref[:, :, lanes].astype(jnp.float32)
        spread = []
        for level in range(levels):
            value = []
            for side in range(2):
                for band in range(bands):
                    first = (side * levels + level) * pairs
                    value.append(held[band, first : first + pairs])
            value = jnp.concatenate(value, axis=0)
            value = (value * turn_cos - swap_pairs(value) * turn_sin).astype(jnp.bfloat16)
            spread.append(
                lax.dot_general(value, tile, (((0,), (0,)), ((), ())), preferred_element_type=jnp.float32)
            )
        for number, first in enumerate(range(0, step, sub)):
            rows = slice(first * 2, (first + sub) * 2)
            part = jnp.concatenate([value[rows] for value in spread], axis=0)
            part_ref[lax.rem(index, 2), number] = jnp.where(keep, part, 0.0).astype(jnp.bfloat16)

    def multiply(index):
        for number, first in enumerate(range(0, step, sub)):
            local = pl.ds(index * step + first, sub)
            table = masked_table(
                leg_ref[local].reshape(sub * heights, degrees), limit_ref[(index * step + first) // sub]
            )
            total = jnp.dot(part_ref[lax.rem(index, 2), number], table, preferred_element_type=jnp.float32)
            out_ref[:, local] = total.astype(jnp.bfloat16).reshape(levels, sub, 2, degrees)

    prepare(0)

    def chunk(index, carry):
        multiply(index)
        prepare(index + 1)
        copy(index).start()
        return carry

    lax.fori_loop(0, chunks - 1, chunk, 0)
    multiply(chunks - 1)
    copy(chunks - 1).start()
    for index in range(chunks):
        copy(index).wait()


def analysis_call(coef, leg, limit, turn, shape):
    levels, slots, _, degrees = shape
    heights = leg.shape[1]
    step, sub = slot_step(slots, heights)
    return pl.pallas_call(
        analysis_kernel,
        in_specs=[VMEM] * 4,
        out_specs=LOOSE,
        out_shape=pltpu.HBM(shape, jnp.bfloat16),
        scratch_shapes=[
            pltpu.VMEM(shape, jnp.bfloat16),
            pltpu.VMEM((2, step // sub, levels * sub * 2, 2 * sub * heights), jnp.bfloat16),
            pltpu.SemaphoreType.DMA((slots // step,)),
        ],
        name="analysis",
        compiler_params=pltpu.CompilerParams(vmem_limit_bytes=20 * MIB),
    )(coef, leg, limit, turn)


def fill_table(waves_ref, table_ref, lon_count, first, last):
    period = 2 * lon_count
    rows = table_ref.shape[0]
    back = 1.5 * lon_count
    row = lax.broadcasted_iota(jnp.int32, (8, LANES), 0).astype(jnp.float32)
    part = lax.broadcasted_iota(jnp.int32, (8, LANES), 1) % 2
    shift = part.astype(jnp.float32) * (lon_count // 2)

    def column(index, carry):
        lanes = pl.ds(pl.multiple_of(index * LANES, LANES), LANES)
        wave = jnp.broadcast_to(waves_ref[0:1, lanes], (8, LANES))
        near = wave * (2.0 * row + 1.0)
        near_cos, near_sin = cos_turn(near, period), cos_turn(near + back, period)
        middle = wave * (16.0 * row)
        middle_cos, middle_sin = cos_turn(middle, period), cos_turn(middle + back, period)
        fine = []
        for j in range(8):
            c, s = middle_cos[j : j + 1], middle_sin[j : j + 1]
            fine.append((near_cos * c - near_sin * s, near_sin * c + near_cos * s))
        for group in range(-(-rows // 512)):
            far = wave * (128.0 * (row + 8.0 * group)) + shift
            far_cos, far_sin = cos_turn(far, period), cos_turn(far + back, period)
            for n in range(8):
                c, s = far_cos[n : n + 1], far_sin[n : n + 1]
                for j in range(0, 8, 2):
                    first = (group * 8 + n) * 64 + j * 8
                    if first < rows:
                        block = [fine[i][0] * c - fine[i][1] * s for i in (j, j + 1)]
                        table_ref[first : first + 16, lanes] = jnp.concatenate(block).astype(jnp.bfloat16)
        return carry

    lax.fori_loop(first, last, column, 0)


def fill_waves(order_ref, waves_ref):
    wave = order_ref[...].astype(jnp.float32).reshape(order_ref.shape[0] // LANES, LANES)
    high = jnp.floor(wave * (1.0 / 256.0))
    digits = (high.astype(jnp.bfloat16), (wave - 256.0 * high).astype(jnp.bfloat16))
    for half in range(2):
        source = iota((LANES, LANES), 1) // 2 + half * (LANES // 2)
        twice = jnp.where(iota((LANES, LANES), 0) == source, 1.0, 0.0).astype(jnp.bfloat16)
        high, low = [jnp.dot(digit, twice, preferred_element_type=jnp.float32) for digit in digits]
        value = high * 256.0 + low
        for r in range(wave.shape[0]):
            first = (2 * r + half) * LANES
            waves_ref[0:1, first : first + LANES] = value[r : r + 1]


def fill_gain(traj_ref, exp_ref, order_ref, gain_ref, scale):
    levels, lat_rows, lon_count = traj_ref.shape
    quarter = lon_count // NBLK
    half = quarter // 2
    rows = levels * lat_rows
    pairs = lat_rows // 2
    padded = gain_ref.shape[1]
    stored = jnp.concatenate([traj_ref[r].astype(jnp.float32) for r in range(levels)], axis=0)
    stored = stored.astype(jnp.bfloat16)
    turned = iota((LANES, LANES), 0) + iota((LANES, LANES), 1) == LANES - 1
    turned = jnp.where(turned, 1.0, 0.0).astype(jnp.bfloat16)
    row, column = iota((rows, rows), 0), iota((rows, rows), 1)
    held = jnp.zeros((rows, rows), jnp.int32)
    for r in range(levels):
        held = jnp.where(column // lat_rows == r, order_ref[0, r], held)
    lat = 2 * (row % pairs) + row // (levels * pairs)
    hit = (held == row // pairs % levels) & (column % lat_rows == lat)
    for block in range(NBLK):
        power = jnp.zeros((rows, rows), jnp.int32)
        for r in range(levels):
            for q in range(lat_rows):
                power = jnp.where(column == r * lat_rows + q, exp_ref[r, q, block], power)
        factor = jnp.where(power < 0, jnp.where(power == -1, 0.5, 0.25), jnp.where(power == 0, 1.0, 2.0))
        factor = jnp.where(power == 2, 4.0, factor)
        pick = jnp.where(hit, factor, 0.0).astype(jnp.bfloat16)
        for reverse in range(2):
            if reverse:
                last = (block + 1) * quarter - 1
                stop = last // LANES + 1
                skip = stop * LANES - 1 - last
                tiles = -(-(skip + half) // LANES)
                tile = stop - tiles
            else:
                tile = block * quarter // LANES
                skip = block * quarter - tile * LANES
                tiles = -(-(skip + half) // LANES)
                stop = tile + tiles
            window = stored[:, tile * LANES : min(stop * LANES, lon_count)]
            if stop * LANES > lon_count:
                fill = jnp.zeros((rows, stop * LANES - lon_count), jnp.bfloat16)
                window = jnp.concatenate([window, fill], axis=1)
            value = jnp.dot(pick, window, preferred_element_type=jnp.float32)
            if reverse:
                value = value.astype(jnp.bfloat16)
                stack = [value[:, t * LANES : (t + 1) * LANES] for t in reversed(range(tiles))]
                value = jnp.dot(jnp.concatenate(stack, axis=0), turned, preferred_element_type=jnp.float32)
                value = jnp.concatenate([value[t * rows : (t + 1) * rows] for t in range(tiles)], axis=1)
            value = (1.0 + jnp.tanh(value[:, skip : skip + half])) * scale
            face = block + (NBLK if (block + reverse) % 2 else 0)
            value = jnp.concatenate([value, jnp.zeros((rows, padded - half), jnp.float32)], axis=1)
            gain_ref[face * rows : (face + 1) * rows] = value


def grid_kernel(
    sizes,
    x_hbm,
    leg_hbm,
    wave_hbm,
    traj_hbm,
    weight_hbm,
    exp_hbm,
    order_hbm,
    coef_hbm,
    out_ref,
    leg_ref,
    limit_ref,
    turn_ref,
    x_ref,
    kept_ref,
    mine_ref,
    total_ref,
    wave_of_ref,
    traj_ref,
    slot_ref,
    weight_ref,
    exp_ref,
    order_ref,
    coef_ref,
    held_ref,
    sums_ref,
    pair_refs,
    lower_refs,
    back_ref,
    waves_ref,
    table_ref,
    gain_ref,
    x_sem,
    leg_sem,
    small_sem,
    mine_sem,
    held_sem,
    sums_send,
    sums_sem,
    pair_send,
    lower_sem,
    back_send,
    back_sem,
):
    levels, pairs, scale = sizes
    bands, rows, width = mine_ref.shape
    lon_count = traj_ref.shape[2]
    groups = lower_refs[0].shape[0]
    parts = total_parts(x_ref.shape[1], leg_ref.shape[1])
    band, lev = lax.axis_index("band"), lax.axis_index("lev")
    group, core = lev // 2, lev % 2

    def there(ahead):
        return lax.rem(band + ahead, bands)

    barrier = pltpu.get_barrier_semaphore()
    small = ((wave_hbm, slot_ref), (weight_hbm, weight_ref), (coef_hbm, coef_ref), (wave_hbm, wave_of_ref))
    small += ((traj_hbm, traj_ref), (exp_hbm, exp_ref), (order_hbm, order_ref))
    small = [pltpu.make_async_copy(source, ref, small_sem.at[n]) for n, (source, ref) in enumerate(small)]
    for copy in small:
        copy.start()
    step, _ = slot_step(x_ref.shape[1], leg_ref.shape[1])

    def copies(index):
        part = pl.ds(index * step, step)
        return (
            pltpu.make_async_copy(x_hbm.at[:, part], x_ref.at[:, part], x_sem.at[index]),
            pltpu.make_async_copy(leg_hbm.at[part], leg_ref.at[part], leg_sem.at[index]),
        )

    def start(index):
        for copy in copies(index):
            copy.start()

    def arrive(index):
        for copy in copies(index):
            copy.wait()

    def shadow():
        for copy in small[3:]:
            copy.wait()
        fill_gain(traj_ref, exp_ref, order_ref, gain_ref, scale)
        fill_waves(wave_of_ref, waves_ref)

    def first():
        for ahead in range(bands):
            for side in range(2):
                if ahead or side:
                    pl.semaphore_signal(
                        barrier,
                        inc=1,
                        device_id={"band": there(ahead), "lev": group * 2 + (core + side) % 2},
                        device_id_type=MESH,
                    )
        for ahead in range(1, groups):
            pl.semaphore_signal(
                barrier,
                inc=1,
                device_id={"band": band, "lev": lax.rem(group + ahead, groups) * 2 + core},
                device_id_type=MESH,
            )
        for copy in small[:3]:
            copy.wait()

    def totals_out(part):
        lanes = parts[part]
        return [
            pltpu.make_async_remote_copy(
                src_ref=total_ref.at[there(ahead), :, lanes],
                dst_ref=sums_ref.at[core, band, :, lanes],
                send_sem=sums_send.at[part, side, ahead],
                recv_sem=sums_sem.at[part, core, band],
                device_id={"band": there(ahead), "lev": group * 2 + (core + side) % 2},
                device_id_type=MESH,
            )
            for ahead in range(bands)
            for side in range(2)
            if ahead or side
        ]

    def send_totals(part):
        lanes = parts[part]
        for copy in totals_out(part):
            copy.start()
        pltpu.make_async_copy(
            total_ref.at[band, :, lanes], sums_ref.at[core, band, :, lanes], sums_sem.at[part, core, band]
        ).start()

    def upper_out(part):
        return [
            pltpu.make_async_remote_copy(
                src_ref=pair_refs[part],
                dst_ref=lower_refs[part].at[group],
                send_sem=pair_send.at[part, ahead],
                recv_sem=lower_sem.at[part, group],
                device_id={"band": band, "lev": jnp.minimum(group + ahead, groups - 1) * 2 + core},
                device_id_type=MESH,
            )
            for ahead in range(1, groups)
        ]

    def pass_up(part):
        lanes = parts[part]
        for source in range(bands):
            for side in range(2):
                pltpu.make_async_copy(
                    total_ref.at[source, :, lanes], sums_ref.at[side, source, :, lanes], sums_sem.at[part, side, source]
                ).wait()
        pair = []
        for source in range(bands):
            both = [sums_ref[side, source, :, lanes].astype(jnp.float32) for side in range(2)]
            pair.append((both[0] + both[1]).astype(jnp.bfloat16))
        pair_refs[part][...] = jnp.concatenate(pair, axis=1)
        for ahead, copy in reversed(list(enumerate(upper_out(part), 1))):

            @pl.when(group + ahead < groups)
            def _():
                copy.start()

    def early():
        pl.semaphore_wait(barrier, 2 * bands - 1 + groups - 1)
        send_totals(0)

    synthesize(
        lon_count,
        mine_ref,
        total_ref,
        leg_ref,
        limit_ref,
        turn_ref,
        x_ref,
        kept_ref,
        slot_ref,
        weight_ref,
        coef_ref,
        start,
        arrive,
        first,
        early,
    )
    if len(parts) == 1:
        early()
    else:
        send_totals(1)
    sends = [
        pltpu.make_async_remote_copy(
            src_ref=mine_ref.at[there(ahead)],
            dst_ref=held_ref.at[band],
            send_sem=mine_sem.at[ahead],
            recv_sem=held_sem.at[band],
            device_id={"band": there(ahead), "lev": lev},
            device_id_type=MESH,
        )
        for ahead in range(1, bands)
    ]
    for copy in sends:
        copy.start()
    pltpu.make_async_copy(mine_ref.at[band], held_ref.at[band], held_sem.at[band]).start()
    if len(parts) > 1:
        pass_up(0)
    shadow()
    columns = table_ref.shape[1] // LANES
    ready = columns * 10 // 20
    fill_table(waves_ref, table_ref, lon_count, 0, ready)
    pass_up(len(parts) - 1)
    fill_table(waves_ref, table_ref, lon_count, ready, columns)

    wave = waves_ref[...]
    part = iota(wave.shape, 1) % 2
    sign_c = 1.0 - 2.0 * part.astype(jnp.float32)
    sign_m = 1.0 - 2.0 * (wave - 2.0 * jnp.floor(wave * 0.5))
    phase = wave - 4.0 * jnp.floor(wave * 0.25)
    stay = jnp.where(phase == 0.0, sign_c, jnp.where(phase == 2.0, -sign_c, 0.0))
    move = jnp.where(phase == 1.0, -1.0, jnp.where(phase == 3.0, 1.0, 0.0))
    signs = (sign_m * sign_c, sign_m, sign_c)

    for source in range(bands):
        pltpu.make_async_copy(mine_ref.at[source], held_ref.at[source], held_sem.at[source]).wait()
    above = jnp.concatenate([sums_ref[0, source] for source in range(bands)], axis=1).astype(jnp.float32)
    above = jnp.where(core == 1, above, 0.0)
    for below in range(groups - 1):
        pieces = []
        for part, (pair_ref, lower_ref) in enumerate(zip(pair_refs, lower_refs)):

            @pl.when(below < group)
            def _():
                pltpu.make_async_copy(pair_ref, lower_ref.at[below], lower_sem.at[part, below]).wait()

            @pl.when(below >= group)
            def _():
                lower_ref[below] = jnp.zeros(lower_ref.shape[1:], jnp.bfloat16)

            piece = lower_ref[below].astype(jnp.float32)
            size = piece.shape[1] // bands
            pieces.append([piece[:, source * size : (source + 1) * size] for source in range(bands)])
        above = above + jnp.concatenate([piece[source] for source in range(bands) for piece in pieces], axis=1)
    scaled = [
        above[side * pairs : (side + 1) * pairs] * coef_ref[level]
        for side in range(2)
        for level in range(levels)
    ]
    value = jnp.concatenate([held_ref[source] for source in range(bands)], axis=1).astype(jnp.float32)
    value = value + jnp.concatenate(scaled, axis=0)
    same, other = value * stay, swap_pairs(value) * move
    far, near = same + other, same - other
    faces = [value] + [value * sign for sign in signs]
    faces += [far, near * signs[0], far * signs[1], near * signs[2]]
    faces = jnp.concatenate([face.astype(jnp.bfloat16) for face in faces], axis=0)
    grid = lax.dot_general(faces, table_ref[...], TO_LANES, preferred_element_type=jnp.float32)
    forcing = (gain_ref[...] * grid).astype(jnp.bfloat16)
    back = jnp.dot(forcing, table_ref[...], preferred_element_type=jnp.float32)
    back = [back[face * rows : (face + 1) * rows] for face in range(2 * NBLK)]
    total = back[0] + back[1] * signs[0] + back[2] * signs[1] + back[3] * signs[2]
    even = back[4] + back[6] * signs[1]
    odd = back[5] * signs[0] + back[7] * signs[2]
    total = total + (even + odd) * stay + swap_pairs(even - odd) * move
    total = total * scale
    half = rows // 2
    both = jnp.concatenate([total[:half] + total[half:], total[:half] - total[half:]], axis=0)
    both = both.astype(jnp.bfloat16)
    for target in range(bands):
        back_ref[target] = both[:, target * width : (target + 1) * width]
    returns = [
        pltpu.make_async_remote_copy(
            src_ref=back_ref.at[there(ahead)],
            dst_ref=out_ref.at[band],
            send_sem=back_send.at[ahead],
            recv_sem=back_sem.at[band],
            device_id={"band": there(ahead), "lev": lev},
            device_id_type=MESH,
        )
        for ahead in range(1, bands)
    ]
    for copy in returns:
        copy.start()
    pltpu.make_async_copy(back_ref.at[band], out_ref.at[band], back_sem.at[band]).start()
    for source in range(bands):
        pltpu.make_async_copy(back_ref.at[source], out_ref.at[source], back_sem.at[source]).wait()
    for copy in sends + returns:
        copy.wait_send()
    for part in range(len(parts)):
        for copy in totals_out(part):
            copy.wait_send()
        for ahead, copy in enumerate(upper_out(part), 1):

            @pl.when(group + ahead < groups)
            def _():
                copy.wait_send()


def grid_call(adj_spec, legendre, wave_of_slot, traj, lat_weight, traj_exp, traj_order, lev_coef):
    levels, slots, _, degrees = adj_spec.shape
    heights = legendre.shape[1]
    step, sub = slot_step(slots, heights)
    lat_rows, lon_count = traj.shape[1:]
    bands = lax.axis_size("band")
    groups = lax.axis_size("lev") // 2
    pairs = lat_rows // 2
    rows = levels * lat_rows
    mine = (bands, rows, slots * 2)
    total = (bands, lat_rows, slots * 2)
    count = bands * slots * 2
    half = lon_count // (2 * NBLK)
    padded = -(-half // 16) * 16
    chunks = slots // step
    sizes = [part.stop - part.start for part in total_parts(slots, heights)]
    scale = 1.0 / math.sqrt(count // 2)
    dma = pltpu.SemaphoreType.DMA
    bf16 = jnp.bfloat16
    operands = (adj_spec, legendre, wave_of_slot, traj, lat_weight, traj_exp, traj_order, lev_coef)
    return pl.pallas_call(
        functools.partial(grid_kernel, (levels, pairs, scale)),
        in_specs=[LOOSE] * 8,
        out_specs=(VMEM,) * 4,
        out_shape=(
            pltpu.VMEM(mine, bf16),
            pltpu.VMEM(legendre.shape, bf16),
            pltpu.VMEM((slots // sub, sub * heights, LANES), jnp.int16),
            pltpu.VMEM((2, slots * 2), jnp.float32),
        ),
        scratch_shapes=[
            pltpu.VMEM(adj_spec.shape, bf16),
            pltpu.VMEM((2, step // sub, levels * sub * 2, 2 * sub * heights), bf16),
            pltpu.VMEM(mine, bf16),
            pltpu.VMEM(total, bf16),
            pltpu.VMEM(wave_of_slot.shape, jnp.int32),
            pltpu.VMEM(traj.shape, bf16),
            pltpu.SMEM(wave_of_slot.shape, jnp.int32),
            pltpu.SMEM(lat_weight.shape, jnp.float32),
            pltpu.SMEM(traj_exp.shape, jnp.int32),
            pltpu.SMEM(traj_order.shape, jnp.int32),
            pltpu.SMEM(lev_coef.shape, jnp.float32),
            pltpu.VMEM(mine, bf16),
            pltpu.VMEM((2,) + total, bf16),
            [pltpu.VMEM((lat_rows, bands * size), bf16) for size in sizes],
            [pltpu.VMEM((groups, lat_rows, bands * size), bf16) for size in sizes],
            pltpu.VMEM(mine, bf16),
            pltpu.VMEM((1, count), jnp.float32),
            pltpu.VMEM((padded, count), bf16),
            pltpu.VMEM((2 * NBLK * rows, padded), jnp.float32),
            dma((chunks,)),
            dma((chunks,)),
            dma((7,)),
            dma((bands,)),
            dma((bands,)),
            dma((len(sizes), 2, bands)),
            dma((len(sizes), 2, bands)),
            dma((len(sizes), groups)),
            dma((len(sizes), groups)),
            dma((bands,)),
            dma((bands,)),
        ],
        name="grid",
        compiler_params=pltpu.CompilerParams(collective_id=0, has_side_effects=True, vmem_limit_bytes=24 * MIB),
    )(*[in_hbm(value) for value in operands])


def body(adj_spec, wave_of_slot, legendre, lat_weight, traj, traj_exp, traj_order, lev_coef):
    coef, leg, limit, turn = grid_call(
        adj_spec, legendre, wave_of_slot, traj, lat_weight, traj_exp, traj_order, lev_coef
    )
    return analysis_call(coef, leg, limit, turn, adj_spec.shape)


def solution(mesh):
    placed = (
        P("lev", "band", None, None),
        P(),
        P("band", None, None),
        P(),
        P("lev", "band", None),
        P("lev", "band", None),
        P("lev", None),
        P("lev"),
    )
    return jax.shard_map(
        body, mesh=mesh, in_specs=placed, out_specs=P("lev", "band", None, None), check_vma=False
    )
```
